256 devices in a mesh: seq: 64 (over z, y, core), mix: 4 (over x).
Axes of the slice: x: 4, y: 4, z: 8, core: 2. Of those that a mesh axis runs over, the one named last changes fastest.
Arguments:
- tokens: bfloat16 [8, 16384, 512], P('mix', 'seq'), may hold values from -6 to 6
- log_forget_rate: bfloat16 [8, 16384, 16], P('mix', 'seq'), may hold values from -0.7 to 0, as said below
- w_x: bfloat16 [512, 1024], P(None, 'mix'), may hold values from -0.25 to 0.25
- w_z: bfloat16 [512, 1024], P(None, 'mix'), may hold values from -0.25 to 0.25
- w_bc: bfloat16 [512, 128], replicated, may hold values from -0.25 to 0.25
- conv_x: bfloat16 [4, 1024], P(None, 'mix'), may hold values from -3 to 3
- conv_bc: bfloat16 [4, 128], replicated, may hold values from -3 to 3
- skip: bfloat16 [16], P('mix'), may hold values from 0.5 to 2
- gain: bfloat16 [1024], P('mix'), may hold values from 0.099609375 to 1.8984375
- w_out: bfloat16 [1024, 512], P('mix'), may hold values from -0.1875 to 0.1875
Outputs:
- mixed: bfloat16 [8, 16384, 512], P('mix', 'seq')
The draws below stay inside these ranges and needn't reach their ends.
Inputs may be any that keep to these rules, and one draw needn't show every extreme that they name: `log_forget_rate`: every entry is below zero.
All inputs are finite; a program needn't handle non-finite values.
Results may differ from the reference program's by a relative error of at most 0.012.
Values may be sent and summed in bfloat16 or wider, within the bound.
No kernel may reach another device: no remote copies, remote signals or barrier semaphores. Data moves between devices by JAX's collectives and lax.ppermute only.
A program may use at most 128 MiB of HBM per device.

```python
import math
import jax
import jax.numpy as jnp
from jax import lax

D = 512
HEADS = 16
HEAD_DIM = 64
STATE = 64
CONV = 4
BLOCK = 128
TOK_DEV = 256
D_INNER = 1024
MIXES = 8
LENGTH = 16384


def draw_log_forget_rate(key, part):
    keys = jax.random.split(key, 6)
    slow_share = 0.5
    slow = jax.random.uniform(keys[0], (MIXES, 1, HEADS)) < slow_share
    fast_rate = jnp.exp(jax.random.uniform(keys[1], (MIXES, 1, HEADS), jnp.float32, math.log(1.0 / 50.0), math.log(1.0 / 20.0)))
    rate = jnp.where(slow, 0.5 / LENGTH, fast_rate)
    rough = jnp.exp(jax.random.uniform(keys[2], (MIXES, LENGTH, HEADS), jnp.float32, math.log(0.5), math.log(2.0)))
    blocks = LENGTH // TOK_DEV
    per_block = jnp.exp(jax.random.uniform(keys[3], (MIXES, blocks, 1, HEADS), jnp.float32, math.log(0.5), math.log(2.0)))
    per_block = jnp.broadcast_to(per_block, (MIXES, blocks, TOK_DEV, HEADS)).reshape(MIXES, LENGTH, HEADS)
    values = -rate * rough * per_block
    spots = jax.random.randint(keys[4], (MIXES, 2), 0, LENGTH)
    where_hit = jnp.any(jnp.arange(LENGTH)[None, :, None] == spots[:, None, :], axis=-1)
    strength = jax.random.uniform(keys[5], (MIXES, LENGTH, HEADS), jnp.float32, 0.25, 0.7)
    values = jnp.where(where_hit[:, :, None], jnp.minimum(values, -strength), values)
    return values.astype(jnp.bfloat16)


def levels(stream_key, dims, pieces, smallest, top_value):
    def one(axis_at, parts):
        heights = jax.random.uniform(jax.random.fold_in(jax.random.fold_in(stream_key, 6), axis_at), (parts,), jnp.float32, smallest / len(pieces), top_value / len(pieces))
        return jnp.repeat(jnp.exp(heights), dims[axis_at] // parts).reshape((-1,) + (1,) * (len(dims) - axis_at - 1))

    loudness = one(*pieces[0])
    for cut in pieces[1:]:
        loudness = loudness * one(*cut)
    return loudness


def centred(own_key, dims, scale, most, cuts=(), dtype=jnp.bfloat16):
    values = scale * jax.random.normal(own_key, dims, jnp.float32)
    if cuts:
        values = values * levels(own_key, dims, cuts, -0.22, 0.18)
    return jnp.clip(values, -most, most).astype(dtype)


def setup_inputs(seed: int = 0) -> dict:
    key_list = jax.random.split(jax.random.key(seed), 11)
    tokens = centred(key_list[0], (MIXES, LENGTH, D), 1.0, 6.0, ((0, 4), (1, 64)))
    log_forget_rate = draw_log_forget_rate(jax.random.fold_in(key_list[10], 71), 0)
    w_x = centred(key_list[2], (D, D_INNER), D ** -0.5, 0.25, ((1, 4),))
    w_z = centred(key_list[3], (D, D_INNER), D ** -0.5, 0.25, ((1, 4),))
    w_bc = centred(key_list[4], (D, 2 * STATE), D ** -0.5, 0.25)
    conv_x = centred(key_list[5], (CONV, D_INNER), CONV ** -0.5, 3.0, ((1, 4),))
    conv_bc = centred(key_list[6], (CONV, 2 * STATE), CONV ** -0.5, 3.0)
    skip = jnp.clip(0.5 + 1.5 * jax.random.uniform(key_list[7], (HEADS,), jnp.float32) ** levels(key_list[7], (HEADS,), ((0, 4),), -0.2, 0.2), 0.5, 2.0).astype(jnp.bfloat16)
    gain = jnp.clip(1.0 + 0.18 * jax.random.normal(key_list[8], (D_INNER,), jnp.float32), 0.099609375, 1.8984375).astype(jnp.bfloat16)
    w_out = centred(key_list[9], (D_INNER, D), D_INNER ** -0.5, 0.1875, ((0, 4),))
    return dict(tokens=tokens, log_forget_rate=log_forget_rate, w_x=w_x, w_z=w_z, w_bc=w_bc, conv_x=conv_x, conv_bc=conv_bc, skip=skip, gain=gain, w_out=w_out)


def conv_silu(pre, taps):
    length = pre.shape[0]
    padded_sequence = jnp.pad(pre.astype(jnp.float32), ((CONV - 1, 0), (0, 0)))
    total = jnp.zeros((length, pre.shape[1]), jnp.float32)
    for k in range(CONV):
        total = total + taps[k].astype(jnp.float32)[None, :] * padded_sequence[k:k + length]
    return jax.nn.silu(total).astype(jnp.bfloat16)

def reference(tokens, log_forget_rate, w_x, w_z, w_bc, conv_x, conv_bc, skip, gain, w_out):
    mask = jnp.tril(jnp.ones((BLOCK, BLOCK), bool))[:, :, None]
    skip_f = skip.astype(jnp.float32)
    gain_f = gain.astype(jnp.float32).reshape(HEADS, HEAD_DIM)

    def one_mixture(item):
        tok, decay = item
        pre_x = jnp.dot(tok, w_x, preferred_element_type=jnp.float32).astype(jnp.bfloat16)
        pre_bc = jnp.dot(tok, w_bc, preferred_element_type=jnp.float32).astype(jnp.bfloat16)
        gate_pre = jnp.dot(tok, w_z, preferred_element_type=jnp.float32).astype(jnp.bfloat16)
        x_act = conv_silu(pre_x, conv_x)
        activated_input_readout = conv_silu(pre_bc, conv_bc)
        count = LENGTH // BLOCK
        blocks = (x_act.reshape(count, BLOCK, HEADS, HEAD_DIM), activated_input_readout[:, :STATE].reshape(count, BLOCK, STATE), activated_input_readout[:, STATE:].reshape(count, BLOCK, STATE), decay.astype(jnp.float32).reshape(count, BLOCK, HEADS), gate_pre.reshape(count, BLOCK, HEADS, HEAD_DIM))

        def step(state, blk):
            xb, input_projection_rows, readout_projection_rows, ab, zb = blk
            cum = jnp.cumsum(ab, axis=0)
            scale_in = jnp.sqrt(-jnp.expm1(2.0 * ab))
            attention_scores = jnp.dot(readout_projection_rows, input_projection_rows.T, preferred_element_type=jnp.float32)
            seg = cum[:, None, :] - cum[None, :, :]
            decay_mat = jnp.where(mask, jnp.exp(jnp.where(mask, seg, -jnp.inf)), 0.0)
            weights = (decay_mat * scale_in[None, :, :] * attention_scores[:, :, None]).astype(jnp.bfloat16)
            xf = xb.astype(jnp.float32)
            intra = jnp.einsum('qkh,khp->qhp', weights.astype(jnp.float32), xf)
            inter = jnp.exp(cum)[:, :, None] * jnp.einsum('qn,hpn->qhp', readout_projection_rows.astype(jnp.float32), state, precision=lax.Precision.HIGHEST)
            tail = jnp.exp(cum[-1][None, :] - cum) * scale_in
            scaled = (xf * tail[:, :, None]).astype(jnp.bfloat16)
            block_state = jnp.einsum('khp,kn->hpn', scaled.astype(jnp.float32), input_projection_rows.astype(jnp.float32))
            new_state = jnp.exp(cum[-1])[:, None, None] * state + block_state
            y = intra + inter + skip_f[None, :, None] * xf
            v = y * jax.nn.silu(zb.astype(jnp.float32))
            normed = v * lax.rsqrt(lax.optimization_barrier(jnp.mean(v * v, axis=-1, keepdims=True)) + 1e-05) * gain_f[None]
            normed = normed.astype(jnp.bfloat16).reshape(BLOCK, HEADS * HEAD_DIM)
            out = jnp.dot(normed, w_out, preferred_element_type=jnp.float32).astype(jnp.bfloat16)
            return (new_state, out)
        init = jnp.zeros((HEADS, HEAD_DIM, STATE), jnp.float32)
        final, outs = lax.scan(step, init, blocks)
        return outs.reshape(LENGTH, outs.shape[-1])
    return lax.map(one_mixture, (tokens, log_forget_rate))
```

```python
import functools

import jax
import jax.numpy as jnp
from jax import lax
from jax.experimental import pallas as pl
from jax.experimental.pallas import tpu as pltpu
from jax.sharding import Mesh
from jax.sharding import PartitionSpec as P

F32, BF16 = jnp.float32, jnp.bfloat16
SEQ = ("seq_0", "seq_1", "seq_2")
STATE = 64
CONV = 4
BLOCK = 128
LANES = 128
HALO = 16
SHARDS = 4


def dot(a, b):
    return jnp.dot(a, b, preferred_element_type=F32)


def hi_lo(value):
    high = value.astype(BF16)
    low = (value - high.astype(F32)).astype(BF16)
    return jnp.concatenate([high, low], axis=-1)


def lower_ones(size):
    rows = lax.broadcasted_iota(jnp.int32, (size, size), 0)
    columns = lax.broadcasted_iota(jnp.int32, (size, size), 1)
    return (rows >= columns).astype(F32).astype(BF16)


def scale_of(rate):
    z = 2.0 * rate
    series = z * (
        1.0
        + z * (1 / 2 + z * (1 / 6 + z * (1 / 24 + z * (1 / 120 + z * (1 / 720)))))
    )
    return jnp.sqrt(jnp.maximum(-jnp.where(z > -0.25, series, jnp.exp(z) - 1.0), 0.0))


def silu(value):
    return value * jax.nn.sigmoid(value)


def conv_silu(halo_rows, rows, taps):
    both = jnp.concatenate([halo_rows, rows], axis=0).astype(BF16).astype(F32)
    total = taps[CONV - 1 : CONV] * both
    for back in range(1, CONV):
        total = total + taps[CONV - 1 - back : CONV - back] * pltpu.roll(both, back, 0)
    return silu(total[HALO:]).astype(BF16)


def prepare_kernel(x_ref, tok_ref, halo_ref, log_ref, wbc_ref, cbc_ref, bc_ref, bt_ref, logp_ref, tail_ref, lmsg_ref, spread_ref):
    mixes, length, _ = tok_ref.shape
    heads = log_ref.shape[2]
    mine = x_ref[0]
    row = lax.broadcasted_iota(jnp.int32, (heads, LANES), 0)
    column = lax.broadcasted_iota(jnp.int32, (heads, LANES), 1)
    per = heads // SHARDS
    source = per * ((mine - column // per + SHARDS) & (SHARDS - 1)) + column % per
    order = jnp.where((row == source) & (column < heads), 1.0, 0.0).astype(BF16)
    width = spread_ref.shape[1]
    head_row = lax.broadcasted_iota(jnp.int32, (2 * LANES, width), 0) & (LANES - 1)
    channel = lax.broadcasted_iota(jnp.int32, (2 * LANES, width), 1)
    spread_ref[...] = jnp.where(head_row == (channel >> 6), 1.0, 0.0).astype(BF16)
    lower = lower_ones(length)
    taps = cbc_ref[...].astype(F32)
    for m in range(mixes):
        rate = dot(log_ref[m], order)
        logp = rate.astype(BF16)
        logp_ref[m] = logp
        cum = dot(lower, logp)
        total = cum[length - 1 : length]
        tail = jnp.exp(total - cum) * scale_of(rate)
        tail_ref[m] = dot(hi_lo(tail), spread_ref[...])
        total_x = dot(hi_lo(jnp.broadcast_to(total, (8, LANES))), spread_ref[...])
        pieces = width // LANES
        for j in range(pieces):
            for q in range(4):
                lmsg_ref[(m * pieces + j) * 4 + q] = total_x[0:1, j * LANES : (j + 1) * LANES]
        bc = conv_silu(dot(halo_ref[m], wbc_ref[...]), dot(tok_ref[m], wbc_ref[...]), taps)
        bc_ref[m] = bc
        bt_ref[m] = bc.astype(F32).T.astype(BF16)


def shard_states(weight, taps, tok_ref, halo_ref, tail_ref, bt_ref, xa_ref, msg_ref, r, at):
    mixes, length, _ = tok_ref.shape
    wide = weight.shape[1]
    pieces = tail_ref.shape[2] // LANES
    for m in range(mixes):
        xa = conv_silu(dot(halo_ref[m], weight), dot(tok_ref[m], weight), taps)
        xa_ref[m, :, at : at + wide] = xa
        scaled = (xa.astype(F32) * tail_ref[m, :, r * wide : (r + 1) * wide]).astype(BF16)
        state = dot(bt_ref[m, 0:STATE, :], scaled).astype(BF16)
        for p in range(wide // LANES):
            j = r * (wide // LANES) + p
            for q in range(4):
                msg_ref[(m * pieces + j) * 4 + q] = state[q * 16 : (q + 1) * 16, p * LANES : (p + 1) * LANES]


def own_kernel(tok_ref, halo_ref, tail_ref, bt_ref, w_ref, p_ref, xa_ref, msg_ref):
    taps = p_ref[0:CONV].astype(F32)
    shard_states(w_ref[...], taps, tok_ref, halo_ref, tail_ref, bt_ref, xa_ref, msg_ref, 0, 0)


def put_halves(core, first, second, out_ref, at, rows):
    out_ref[at : at + rows] = jnp.where(core == 0, first, second)
    out_ref[at + rows : at + 2 * rows] = jnp.where(core == 0, second, first)


def others_kernel(c_ref, tok_ref, halo_ref, tail_ref, bt_ref, own_msg_ref, own_p_ref, *rest):
    here, there = rest[0 : SHARDS - 1], rest[SHARDS - 1 : 2 * SHARDS - 2]
    xa_ref, msg_ref, prm_ref, w_ref = rest[2 * SHARDS - 2 :]
    core = c_ref[0]
    mixes = tok_ref.shape[0]
    half = tok_ref.shape[2] // 2
    wide = own_p_ref.shape[1]
    prm_ref[:, 0:wide] = own_p_ref[...]
    span = own_msg_ref.shape[0] // mixes
    for m in range(mixes):
        own = span // SHARDS
        msg_ref[m * span : m * span + own] = own_msg_ref[m * span : m * span + own]
    for r in range(1, SHARDS):
        put_halves(core, here[r - 1][0:half], there[r - 1][0:half], w_ref, 0, half)
        extra = here[r - 1][half : half + 8]
        prm_ref[:, r * wide : (r + 1) * wide] = extra
        shard_states(
            w_ref[...], extra[0:CONV].astype(F32), tok_ref, halo_ref, tail_ref, bt_ref, xa_ref, msg_ref, r, (r - 1) * wide
        )


def scan_kernel(s_ref, l_ref, out_ref):
    def step(k, carry):
        out_ref[k] = carry.astype(BF16)
        return carry * jnp.exp(l_ref[k]) + s_ref[k].astype(F32)

    lax.fori_loop(0, s_ref.shape[0], step, jnp.zeros(s_ref.shape[1:], F32), unroll=8)


def local_kernel(c_ref, tok_ref, xa0_ref, xa1_ref, bc_ref, bt_ref, logp_ref, spread_ref, prm_ref, wz0_ref, wo0_ref, *rest):
    here, there = rest[0 : SHARDS - 1], rest[SHARDS - 1 : 2 * SHARDS - 2]
    yg_ref, eg_ref, wo_ref, wz_ref = rest[2 * SHARDS - 2 :]
    core = c_ref[0]
    mixes, length, depth = tok_ref.shape
    half = depth // 2
    wide = wz0_ref.shape[1]
    wz_ref[0] = wz0_ref[...]
    wo_ref[0:wide] = wo0_ref[...]
    for r in range(1, SHARDS):
        a, b = here[r - 1], there[r - 1]
        wz_ref[r, 0:half] = jnp.where(core == 0, a[0:half], b[0:half])
        wz_ref[r, half:depth] = jnp.where(core == 0, b[0:half], a[0:half])
        q = wide // 2
        for s in range(2):
            part = slice(half + s * q, half + (s + 1) * q)
            lanes = slice(s * wide, (s + 1) * wide)
            wo_ref[r * wide : r * wide + q, lanes] = jnp.where(core == 0, a[part], b[part])
            wo_ref[r * wide + q : (r + 1) * wide, lanes] = jnp.where(core == 0, b[part], a[part])
    blocks = length // BLOCK
    lower_block = lower_ones(BLOCK)
    lower = lower_ones(length)
    keep = lax.broadcasted_iota(jnp.int32, (BLOCK, BLOCK), 0) >= lax.broadcasted_iota(jnp.int32, (BLOCK, BLOCK), 1)
    left = lax.broadcasted_iota(jnp.int32, (BLOCK, LANES), 1) < LANES // 2

    def mixture(m, _):
        logp = logp_ref[m]
        rate = logp.astype(F32)
        scale = scale_of(rate)
        scale_t = scale.T
        cum_dev = dot(lower, logp)
        cums = [dot(lower_block, logp[b * BLOCK : (b + 1) * BLOCK]) for b in range(blocks)]
        cums_t = [cum.T for cum in cums]
        bc = bc_ref[m]
        bt = bt_ref[m]
        reads = [bc[b * BLOCK : (b + 1) * BLOCK, STATE:] for b in range(blocks)]
        writes_t = [bt[0:STATE, b * BLOCK : (b + 1) * BLOCK] for b in range(blocks)]
        scores = [jnp.where(keep, dot(reads[b], writes_t[b]), 0.0) for b in range(blocks)]
        grow = hi_lo(jnp.exp(cum_dev))
        enter = [hi_lo(jnp.exp(cum)) for cum in cums]
        leave = [
            hi_lo(jnp.exp(cums[b][BLOCK - 1 :] - cums[b]) * scale[b * BLOCK : (b + 1) * BLOCK]) for b in range(blocks)
        ]
        last = [jnp.broadcast_to(jnp.exp(cums[b][BLOCK - 1 :]), (8, LANES)) for b in range(blocks)]
        for r in range(SHARDS):
            gate_pre = dot(tok_ref[m], wz_ref[r]).astype(BF16)
            for p in range(wide // LANES):
                j = r * (wide // LANES) + p
                lanes = slice(j * LANES, (j + 1) * LANES)
                gate = silu(gate_pre[:, p * LANES : (p + 1) * LANES].astype(F32))
                spread = spread_ref[:, lanes]
                if r == 0:
                    x = xa0_ref[m, :, lanes]
                else:
                    x = xa1_ref[m, :, j * LANES - wide : (j + 1) * LANES - wide]
                skip = prm_ref[5:6, lanes].astype(F32)
                state = None
                for b in range(blocks):
                    here_rows = slice(b * BLOCK, (b + 1) * BLOCK)
                    xb = x[here_rows]
                    parts = []
                    for h in (2 * j, 2 * j + 1):
                        seg = cums[b][:, h : h + 1] - cums_t[b][h : h + 1, :]
                        decay = jnp.exp(jnp.minimum(seg, 0.0))
                        weights = decay * (scores[b] * scale_t[h : h + 1, here_rows])
                        parts.append(dot(weights.astype(BF16), xb))
                    y = jnp.where(left, parts[0], parts[1]) + skip * xb.astype(F32)
                    if state is not None:
                        y = y + dot(enter[b], spread) * dot(reads[b], state.astype(BF16))
                    if b + 1 < blocks:
                        scaled = (xb.astype(F32) * dot(leave[b], spread)).astype(BF16)
                        fresh = dot(writes_t[b], scaled)
                        if state is not None:
                            fresh = fresh + dot(hi_lo(last[b]), spread)[0:1] * state
                        state = fresh
                    yg_ref[m, here_rows, lanes] = y * gate[here_rows]
                eg_ref[m, :, lanes] = dot(grow, spread) * gate
        return 0

    lax.fori_loop(0, mixes, mixture, 0)


def final_kernel(back_ref, bc_ref, yg_ref, eg_ref, prm_ref, wo_ref, out_ref, normed_ref):
    mixes, length, width = yg_ref.shape
    pieces = width // LANES
    rows = lax.broadcasted_iota(jnp.int32, (2 * LANES, LANES), 0) & (LANES - 1)
    columns = lax.broadcasted_iota(jnp.int32, (2 * LANES, LANES), 1)
    same_head = jnp.where((rows >> 6) == (columns >> 6), 1.0, 0.0).astype(BF16)
    for m in range(mixes):
        read = bc_ref[m][:, STATE:]
        for j in range(pieces):
            lanes = slice(j * LANES, (j + 1) * LANES)
            at = (m * pieces + j) * 4
            carry = jnp.concatenate([back_ref[at + q] for q in range(4)], axis=0)
            v = yg_ref[m, :, lanes] + eg_ref[m, :, lanes] * dot(read, carry)
            mean = dot(hi_lo(v * v), same_head) * (1.0 / 64.0)
            gain = prm_ref[4:5, lanes].astype(F32)
            normed_ref[:, lanes] = (v * lax.rsqrt(mean + 1e-05) * gain).astype(BF16)
        out_ref[m] = dot(normed_ref[...], wo_ref[...]).astype(BF16)


VMEM = pl.BlockSpec(memory_space=pltpu.VMEM)
SMEM = pl.BlockSpec(memory_space=pltpu.SMEM)


def call(kernel, name, outs, args, scratch=(), scalars=0, flops=0, mib=24):
    bytes_accessed = sum(a.size * a.dtype.itemsize for a in args)
    return pl.pallas_call(
        kernel,
        name=name,
        out_shape=[jax.ShapeDtypeStruct(shape, dtype) for shape, dtype in outs],
        in_specs=[SMEM] * scalars + [VMEM] * (len(args) - scalars),
        out_specs=[VMEM] * len(outs),
        scratch_shapes=list(scratch),
        compiler_params=pltpu.CompilerParams(vmem_limit_bytes=mib * 2**20),
        cost_estimate=pl.CostEstimate(flops=flops, bytes_accessed=bytes_accessed, transcendentals=0),
    )(*args)


def around(value, axis, steps):
    count = lax.axis_size(axis)
    return lax.ppermute(value, axis, [(k, (k + steps) % count) for k in range(count)])


def body(tokens, log_forget_rate, w_x, w_z, w_bc, conv_x, conv_bc, skip, gain, w_out):
    core, across = lax.axis_index("seq_2"), lax.axis_index("mix")
    core_s, across_s = core.astype(jnp.int32)[None], across.astype(jnp.int32)[None]
    mixes, length, depth = tokens.shape
    wide = w_x.shape[1]
    width = wide * SHARDS
    half = depth // 2
    count = lax.axis_size(SEQ)

    extra = jnp.concatenate(
        [conv_x, gain[None], jnp.repeat(skip, wide // skip.shape[0])[None], jnp.zeros((2, wide), BF16)], axis=0
    )
    first = jnp.concatenate([lax.dynamic_slice(w_x, (core * half, 0), (half, wide)), extra], axis=0)
    x_here = [around(first, "mix", r) for r in range(1, SHARDS)]
    halo = lax.ppermute(tokens[:, length - HALO :], SEQ, [(k, k + 1) for k in range(count - 1)])
    x_there = [around(part, "seq_2", 1) for part in x_here]

    bc, bt, logp, tail, lmsg, spread = call(
        prepare_kernel,
        "prepare",
        [
            ((mixes, length, 2 * STATE), BF16),
            ((mixes, 2 * STATE, length), BF16),
            ((mixes, length, LANES), BF16),
            ((mixes, length, width), F32),
            ((count, 1, LANES), F32),
            ((2 * LANES, width), BF16),
        ],
        (across_s, tokens, halo, log_forget_rate, w_bc, conv_bc),
        scalars=1,
        flops=2 * 10**8,
    )
    totals = lax.all_to_all(lmsg, SEQ, 0, 0)
    xa0, own_msg = call(
        own_kernel,
        "own",
        [((mixes, length, wide), BF16), ((count, 16, LANES), BF16)],
        (tokens, halo, tail, bt, w_x, extra),
        flops=2 * 10**8,
    )
    xa1, msg, prm = call(
        others_kernel,
        "others",
        [((mixes, length, width - wide), BF16), ((count, 16, LANES), BF16), ((8, width), BF16)],
        (core_s, tokens, halo, tail, bt, own_msg, extra, *x_here, *x_there),
        scratch=[pltpu.VMEM((depth, wide), BF16)],
        scalars=1,
        flops=6 * 10**8,
    )
    arrived = lax.all_to_all(msg, SEQ, 0, 0)

    out_half = lax.dynamic_slice(w_out, (core * (wide // 2), 0), (wide // 2, depth))
    second = jnp.concatenate(
        [lax.dynamic_slice(w_z, (core * half, 0), (half, wide)), out_half[:, :wide], out_half[:, wide:]], axis=0
    )
    second, _ = lax.optimization_barrier((second, x_here))
    z_here = [around(second, "mix", r) for r in range(1, SHARDS)]
    z_there = [around(part, "seq_2", 1) for part in z_here]

    (carries,) = call(scan_kernel, "scan", [((count, 16, LANES), BF16)], (arrived, totals), flops=10**7)
    back = lax.all_to_all(carries, SEQ, 0, 0)
    yg, eg, wo = call(
        local_kernel,
        "local",
        [((mixes, length, width), F32), ((mixes, length, width), F32), ((width, depth), BF16)],
        (core_s, tokens, xa0, xa1, bc, bt, logp, spread, prm, w_z, w_out, *z_here, *z_there),
        scratch=[pltpu.VMEM((SHARDS, depth, wide), BF16)],
        scalars=1,
        flops=2 * 10**9,
    )
    (mixed,) = call(
        final_kernel,
        "final",
        [((mixes, length, depth), BF16)],
        (back, bc, yg, eg, prm, wo),
        scratch=[pltpu.VMEM((length, width), BF16)],
        flops=10**9,
    )
    return mixed


def solution(mesh):
    finer = Mesh(
        mesh.devices.reshape(8, 4, 2, mesh.shape["mix"]), ("seq_0", "seq_1", "seq_2", "mix")
    )
    placed = (
        P("mix", SEQ, None),
        P("mix", SEQ, None),
        P(None, "mix"),
        P(None, "mix"),
        P(),
        P(None, "mix"),
        P(),
        P("mix"),
        P("mix"),
        P("mix", None),
    )
    return jax.shard_map(
        body, mesh=finer, in_specs=placed, out_specs=P("mix", SEQ, None), check_vma=False
    )
```

```python
import jax
import jax.numpy as jnp
from jax import lax
from jax.experimental import pallas as pl
from jax.experimental.pallas import tpu as pltpu
from jax.sharding import Mesh
from jax.sharding import PartitionSpec as P

F32, BF16 = jnp.float32, jnp.bfloat16
CHIPS = ("seq_0", "seq_1")
SEQ = ("seq_0", "seq_1", "seq_2")
STATE = 64
CONV = 4
BLOCK = 128
LANES = 128
HALO = 16
SHARDS = 4
PART = 16


def dot(a, b):
    return jnp.dot(a, b, preferred_element_type=F32)


def iota(shape, axis):
    return lax.broadcasted_iota(jnp.int32, shape, axis)


def ones_where(mask):
    return jnp.where(mask, 1.0, 0.0).astype(BF16)


def hi_lo(value):
    high = value.astype(BF16)
    low = (value - high.astype(F32)).astype(BF16)
    return jnp.concatenate([high, low], axis=-1)


def lower_ones(size):
    return ones_where(iota((size, size), 0) >= iota((size, size), 1))


def spread(start, width):
    shape = (2 * LANES, width)
    return ones_where((iota(shape, 0) & (LANES - 1)) == ((iota(shape, 1) + start) >> 6))


def scale_of(rate):
    z = 2.0 * rate
    series = z * (
        1.0
        + z * (1 / 2 + z * (1 / 6 + z * (1 / 24 + z * (1 / 120 + z * (1 / 720)))))
    )
    return jnp.sqrt(jnp.maximum(-jnp.where(z > -0.25, series, jnp.exp(z) - 1.0), 0.0))


def silu(value):
    return value * jax.nn.sigmoid(value)


def conv_silu(rows, taps):
    rows = rows.astype(BF16).astype(F32)
    total = taps[CONV - 1 : CONV] * rows
    for back in range(1, CONV):
        total = total + taps[CONV - 1 - back : CONV - back] * pltpu.roll(rows, back, 0)
    return silu(total[HALO:]).astype(BF16)


def pack_kernel(c_ref, wx_ref, tok_ref, cx_ref, log_ref, first_ref, send_ref, h0_ref, h1_ref, sems):
    core = c_ref[0]
    half = first_ref.shape[0] - 8
    length = tok_ref.shape[1]
    rows = pl.ds(pl.multiple_of(core * half, half), half)
    copies = [
        pltpu.make_async_copy(wx_ref.at[rows], first_ref.at[0:half], sems.at[0]),
        pltpu.make_async_copy(tok_ref.at[1 - core], send_ref.at[0:length], sems.at[1]),
        pltpu.make_async_copy(tok_ref.at[0, length - HALO : length], h0_ref, sems.at[2]),
        pltpu.make_async_copy(tok_ref.at[1, length - HALO : length], h1_ref, sems.at[3]),
    ]
    for copy in copies:
        copy.start()
    first_ref[half : half + 8] = jnp.concatenate([cx_ref[...].astype(F32)] * 2, axis=0).astype(BF16)
    logs = log_ref[1 - core]
    send_ref[length : length + 16] = jnp.concatenate([logs, logs], axis=1)
    for copy in copies:
        copy.wait()


def shard_states(weight, taps, r, at, tok_ref, tail_ref, bt_ref, xa_ref, msg_ref):
    wide = weight.shape[1]
    xa = conv_silu(dot(tok_ref[...], weight), taps)
    xa_ref[:, at : at + wide] = xa
    tail = dot(tail_ref[...], spread(r * wide, wide))
    state = dot(bt_ref[0:STATE, :], (xa.astype(F32) * tail).astype(BF16)).astype(BF16)
    for p in range(wide // LANES):
        for q in range(STATE // PART):
            at_piece = (r * (wide // LANES) + p) * (STATE // PART) + q
            msg_ref[at_piece, 0:PART] = state[q * PART : (q + 1) * PART, p * LANES : (p + 1) * LANES]


def own_kernel(
    c_ref, x_ref, tokens_ref, log_ref, got_ref, h0_ref, h1_ref, wbc_ref, cbc_ref, w_ref, cx_ref,
    tok_ref, bc_ref, bt_ref, logp_ref, tail_ref, xa_ref, msg_ref, sem,
):
    core, mine = c_ref[0], x_ref[0]
    heads, length = log_ref.shape[1:]
    here = pl.multiple_of(HALO + core * length, HALO)
    there = pl.multiple_of(HALO + (1 - core) * length, HALO)
    copy = pltpu.make_async_copy(tokens_ref.at[core], tok_ref.at[pl.ds(here, length)], sem)
    copy.start()
    tok_ref[pl.ds(there, length)] = got_ref[0:length]
    tok_ref[0:HALO] = h0_ref[...] + h1_ref[...]

    per = heads // SHARDS
    shape = (LANES, heads)
    rel = iota(shape, 0)
    source = per * ((mine - rel // per + SHARDS) & (SHARDS - 1)) + rel % per
    order = ones_where((iota(shape, 1) == source) & (rel < heads))
    a, b = log_ref[core], got_ref[length : length + heads, 0:length]
    logs = jnp.concatenate([jnp.where(core == 0, a, b), jnp.where(core == 0, b, a)], axis=1)
    rate = dot(order, logs).T
    logp = rate.astype(BF16)
    logp_ref[...] = logp
    cum = dot(lower_ones(2 * length), logp)
    total = cum[2 * length - 1 :]
    tail_ref[...] = hi_lo(jnp.exp(total - cum) * scale_of(rate))
    width = SHARDS * w_ref.shape[1]
    total_x = dot(hi_lo(jnp.broadcast_to(total, (8, LANES))), spread(0, width))
    high = total_x.astype(BF16).astype(F32)
    row = iota((8, width), 0)
    extra = jnp.where(row == 0, high, jnp.where(row == 1, total_x - high, 0.0)).astype(BF16)
    parts = STATE // PART
    for j in range(width // LANES):
        for q in range(parts):
            msg_ref[j * parts + q, PART : PART + 8] = extra[:, j * LANES : (j + 1) * LANES]
    copy.wait()
    bc = conv_silu(dot(tok_ref[...], wbc_ref[...]), cbc_ref[...].astype(F32))
    bc_ref[...] = bc
    bt_ref[...] = bc.astype(F32).T.astype(BF16)
    shard_states(w_ref[...], cx_ref[...].astype(F32), 0, 0, tok_ref, tail_ref, bt_ref, xa_ref, msg_ref)


def others_kernel(c_ref, tok_ref, tail_ref, bt_ref, own_msg_ref, *rest):
    here, there = rest[0 : SHARDS - 1], rest[SHARDS - 1 : 2 * SHARDS - 2]
    xa_ref, msg_ref, w_ref = rest[2 * SHARDS - 2 :]
    core = c_ref[0]
    half, wide = w_ref.shape[0] // 2, w_ref.shape[1]
    msg_ref[...] = own_msg_ref[...]
    for r in range(1, SHARDS):
        a, b = here[r - 1][0:half], there[r - 1][0:half]
        w_ref[0:half] = jnp.where(core == 0, a, b)
        w_ref[half : 2 * half] = jnp.where(core == 0, b, a)
        taps = here[r - 1][half : half + 8].astype(F32)
        shard_states(w_ref[...], taps, r, (r - 1) * wide, tok_ref, tail_ref, bt_ref, xa_ref, msg_ref)


def scan_kernel(s_ref, out_ref):
    def step(k, carry):
        out_ref[k] = carry.astype(BF16)
        extra = s_ref[k, PART : PART + 8].astype(F32)
        return carry * jnp.exp(extra[0:1] + extra[1:2]) + s_ref[k, 0:PART].astype(F32)

    lax.fori_loop(0, s_ref.shape[0], step, jnp.zeros((PART, LANES), F32), unroll=8)


def local_kernel(c_ref, tok_ref, xa0_ref, xa1_ref, bc_ref, bt_ref, logp_ref, wz0_ref, wo0_ref, p0_ref, *rest):
    here, there = rest[0 : SHARDS - 1], rest[SHARDS - 1 : 2 * SHARDS - 2]
    yg_ref, eg_ref, wo_ref, gain_ref, wz_ref = rest[2 * SHARDS - 2 :]
    core = c_ref[0]
    depth, wide = wz0_ref.shape
    half, q = depth // 2, wide // 2
    length = bc_ref.shape[0]
    wo_ref[0:wide] = wo0_ref[...]
    blocks = length // BLOCK
    lower_block = lower_ones(BLOCK)
    keep = iota((BLOCK, BLOCK), 0) >= iota((BLOCK, BLOCK), 1)
    left = iota((BLOCK, LANES), 1) < LANES // 2
    bt = bt_ref[...]
    rate = logp_ref[...].astype(F32)
    scale = scale_of(rate)
    scale_t = scale.T
    grow = hi_lo(jnp.exp(dot(lower_ones(length), logp_ref[...])))
    span = [slice(b * BLOCK, (b + 1) * BLOCK) for b in range(blocks)]
    cums = [dot(lower_block, logp_ref[span[b]]) for b in range(blocks)]
    cums_t = [cum.T for cum in cums]
    reads = [bc_ref[span[b]][:, STATE:] for b in range(blocks)]
    writes_t = [bt[0:STATE, b * BLOCK : (b + 1) * BLOCK] for b in range(blocks)]
    scores = [jnp.where(keep, dot(reads[b], writes_t[b]), 0.0) for b in range(blocks)]
    enter = [hi_lo(jnp.exp(cum)) for cum in cums]
    leave = [hi_lo(jnp.exp(cums[b][BLOCK - 1 :] - cums[b]) * scale[span[b]]) for b in range(blocks)]
    last = [hi_lo(jnp.broadcast_to(jnp.exp(cums[b][BLOCK - 1 :]), (8, LANES))) for b in range(blocks)]
    for r in range(SHARDS):
        if r == 0:
            wz_ref[...] = wz0_ref[...]
            extra = p0_ref[...]
        else:
            a, b = here[r - 1], there[r - 1]
            wz_ref[0:half] = jnp.where(core == 0, a[0:half], b[0:half])
            wz_ref[half:depth] = jnp.where(core == 0, b[0:half], a[0:half])
            for s in range(2):
                part = slice(half + s * q, half + (s + 1) * q)
                lanes = slice(s * wide, (s + 1) * wide)
                wo_ref[r * wide : r * wide + q, lanes] = jnp.where(core == 0, a[part], b[part])
                wo_ref[r * wide + q : (r + 1) * wide, lanes] = jnp.where(core == 0, b[part], a[part])
            extra = a[2 * half : 2 * half + 8]
        gain_ref[:, r * wide : (r + 1) * wide] = extra
        gate_pre = dot(tok_ref[HALO:], wz_ref[...]).astype(BF16)
        for p in range(wide // LANES):
            j = r * (wide // LANES) + p
            lanes = slice(j * LANES, (j + 1) * LANES)
            own = slice(p * LANES, (p + 1) * LANES)
            gate = silu(gate_pre[:, own].astype(F32))
            to_lanes = spread(j * LANES, LANES)
            x = xa0_ref[:, lanes] if r == 0 else xa1_ref[:, j * LANES - wide : (j + 1) * LANES - wide]
            skip = extra[1:2, own].astype(F32)
            state = None
            for b in range(blocks):
                xb = x[span[b]]
                parts = []
                for h in (2 * j, 2 * j + 1):
                    seg = cums[b][:, h : h + 1] - cums_t[b][h : h + 1, :]
                    decay = jnp.exp(jnp.minimum(seg, 0.0))
                    weights = decay * (scores[b] * scale_t[h : h + 1, span[b]])
                    parts.append(dot(weights.astype(BF16), xb))
                y = jnp.where(left, parts[0], parts[1]) + skip * xb.astype(F32)
                if state is not None:
                    y = y + dot(enter[b], to_lanes) * dot(reads[b], state.astype(BF16))
                if b + 1 < blocks:
                    scaled = (xb.astype(F32) * dot(leave[b], to_lanes)).astype(BF16)
                    fresh = dot(writes_t[b], scaled)
                    state = fresh if state is None else fresh + dot(last[b], to_lanes)[0:1] * state
                yg_ref[span[b], lanes] = (y * gate[span[b]]).astype(BF16)
            eg_ref[:, lanes] = (dot(grow, to_lanes) * gate).astype(BF16)


def final_rows(start, back_ref, bc_ref, yg_ref, eg_ref, gain_ref, wo_ref, normed_ref):
    length, width = normed_ref.shape
    rows = pl.ds(pl.multiple_of(start, length), length)
    read = bc_ref[rows, :][:, STATE:]
    shape = (2 * LANES, LANES)
    same_head = ones_where(((iota(shape, 0) & (LANES - 1)) >> 6) == (iota(shape, 1) >> 6))
    parts = STATE // PART
    for j in range(width // LANES):
        lanes = slice(j * LANES, (j + 1) * LANES)
        carry = jnp.concatenate([back_ref[j * parts + q] for q in range(parts)], axis=0)
        v = yg_ref[rows, lanes].astype(F32) + eg_ref[rows, lanes].astype(F32) * dot(read, carry)
        mean = dot(hi_lo(v * v), same_head) * (1.0 / 64.0)
        gain = gain_ref[0:1, lanes].astype(F32)
        normed_ref[:, lanes] = (v * lax.rsqrt(mean + 1e-05) * gain).astype(BF16)
    return dot(normed_ref[...], wo_ref[...]).astype(BF16)


def final_send_kernel(c_ref, back_ref, bc_ref, yg_ref, eg_ref, gain_ref, wo_ref, out_ref, normed_ref):
    start = (1 - c_ref[0]) * normed_ref.shape[0]
    out_ref[...] = final_rows(start, back_ref, bc_ref, yg_ref, eg_ref, gain_ref, wo_ref, normed_ref)


def final_own_kernel(c_ref, back_ref, bc_ref, yg_ref, eg_ref, gain_ref, wo_ref, out_ref, normed_ref):
    start = c_ref[0] * normed_ref.shape[0]
    out_ref[...] = final_rows(start, back_ref, bc_ref, yg_ref, eg_ref, gain_ref, wo_ref, normed_ref)


def join_kernel(c_ref, own_ref, got_ref, out_ref, sems):
    core = c_ref[0]
    copies = [
        pltpu.make_async_copy(own_ref, out_ref.at[core], sems.at[0]),
        pltpu.make_async_copy(got_ref, out_ref.at[1 - core], sems.at[1]),
    ]
    for copy in copies:
        copy.start()
    for copy in copies:
        copy.wait()


VMEM = pl.BlockSpec(memory_space=pltpu.VMEM)
SMEM = pl.BlockSpec(memory_space=pltpu.SMEM)
HBM = pl.BlockSpec(memory_space=pltpu.HBM)
ANY = pl.BlockSpec()


def call(kernel, name, outs, args, specs, out_specs=None, scratch=(), flops=0, mib=24):
    return pl.pallas_call(
        kernel,
        name=name,
        out_shape=[jax.ShapeDtypeStruct(shape, dtype) for shape, dtype in outs],
        in_specs=specs,
        out_specs=out_specs or [VMEM] * len(outs),
        scratch_shapes=list(scratch),
        compiler_params=pltpu.CompilerParams(vmem_limit_bytes=mib * 2**20),
        cost_estimate=pl.CostEstimate(flops=flops, bytes_accessed=2**20, transcendentals=0),
    )(*args)


def around(value, axis, steps):
    count = lax.axis_size(axis)
    return lax.ppermute(value, axis, [(k, (k + steps) % count) for k in range(count)])


def body(tokens, log_forget_rate, w_x, w_z, w_bc, conv_x, conv_bc, skip, gain, w_out):
    core, across = lax.axis_index("seq_2"), lax.axis_index("mix")
    core_s, across_s = core.astype(jnp.int32)[None], across.astype(jnp.int32)[None]
    _, length, depth = tokens.shape
    wide = w_x.shape[1]
    width = wide * SHARDS
    half = depth // 2
    chips = lax.axis_size(CHIPS)
    both = 2 * length
    logs = jnp.swapaxes(log_forget_rate, 1, 2)
    heads = logs.shape[1]
    parts = width // LANES * (STATE // PART)

    first, send, h0, h1 = call(
        pack_kernel,
        "pack",
        [((half + 8, wide), BF16), ((length + heads, depth), BF16), ((HALO, depth), BF16), ((HALO, depth), BF16)],
        (core_s, w_x, tokens, conv_x, logs),
        [SMEM, HBM, HBM, ANY, ANY],
        scratch=[pltpu.SemaphoreType.DMA((4,))],
    )
    got = around(send, "seq_2", 1)
    x_here = [around(first, "mix", r) for r in range(1, SHARDS)]
    halo = [
        lax.ppermute(h, SEQ, [(2 * k + 1, 2 * k + 2 + to) for k in range(chips - 1)]) for to, h in enumerate((h0, h1))
    ]
    tok, bc, bt, logp, tail, xa0, own_msg = call(
        own_kernel,
        "own",
        [
            ((HALO + both, depth), BF16),
            ((both, 2 * STATE), BF16),
            ((2 * STATE, both), BF16),
            ((both, LANES), BF16),
            ((both, 2 * LANES), BF16),
            ((both, wide), BF16),
            ((parts, PART + 8, LANES), BF16),
        ],
        (core_s, across_s, tokens, logs, got, *halo, w_bc, conv_bc, w_x, conv_x),
        [SMEM, SMEM, HBM, ANY, VMEM, VMEM, VMEM, ANY, ANY, ANY, ANY],
        scratch=[pltpu.SemaphoreType.DMA],
        flops=10**9,
    )
    (x_here, own_msg) = lax.optimization_barrier((x_here, own_msg))
    x_there = [around(part, "seq_2", 1) for part in x_here]
    xa1, msg = call(
        others_kernel,
        "others",
        [((both, width - wide), BF16), ((parts, PART + 8, LANES), BF16)],
        (core_s, tok, tail, bt, own_msg, *x_here, *x_there),
        [SMEM] + [VMEM] * 10,
        scratch=[pltpu.VMEM((depth, wide), BF16)],
        flops=10**9,
    )
    arrived = lax.all_to_all(msg, CHIPS, 0, 0)

    w_z, w_out, gain, skip, _ = lax.optimization_barrier((w_z, w_out, gain, skip, msg))
    p0 = jnp.concatenate(
        [gain[None], jnp.repeat(skip, wide // skip.shape[0])[None], jnp.zeros((6, wide), BF16)], axis=0
    )
    out_half = lax.dynamic_slice(w_out, (core * (wide // 2), 0), (wide // 2, depth))
    second = jnp.concatenate(
        [lax.dynamic_slice(w_z, (core * half, 0), (half, wide)), out_half[:, :wide], out_half[:, wide:], p0], axis=0
    )
    z_here = [around(second, "mix", r) for r in range(1, SHARDS)]

    (carries,) = call(scan_kernel, "scan", [((parts, PART, LANES), BF16)], (arrived,), [VMEM], flops=10**7)
    z_there = [around(part, "seq_2", 1) for part in z_here]
    back = lax.all_to_all(carries, CHIPS, 0, 0)
    yg, eg, wo, gains = call(
        local_kernel,
        "local",
        [((both, width), BF16), ((both, width), BF16), ((width, depth), BF16), ((8, width), BF16)],
        (core_s, tok, xa0, xa1, bc, bt, logp, w_z, w_out, p0, *z_here, *z_there),
        [SMEM] + [ANY] * 15,
        scratch=[pltpu.VMEM((depth, wide), BF16)],
        flops=2 * 10**9,
    )
    ends = (core_s, back, bc, yg, eg, gains, wo)
    specs = [SMEM, VMEM, ANY, VMEM, VMEM, VMEM, VMEM]
    scratch = [pltpu.VMEM((length, width), BF16)]
    (away,) = call(final_send_kernel, "final_send", [((length, depth), BF16)], ends, specs, scratch=scratch, flops=10**9)
    back_home = around(away, "seq_2", 1)
    (home,) = call(final_own_kernel, "final_own", [((length, depth), BF16)], ends, specs, scratch=scratch, flops=10**9)
    (mixed,) = call(
        join_kernel,
        "join",
        [((2, length, depth), BF16)],
        (core_s, home, back_home),
        [SMEM, VMEM, VMEM],
        out_specs=[HBM],
        scratch=[pltpu.SemaphoreType.DMA((2,))],
    )
    return mixed


def solution(mesh):
    finer = Mesh(
        mesh.devices.reshape(8, 4, 2, mesh.shape["mix"]), ("seq_0", "seq_1", "seq_2", "mix")
    )
    placed = (
        P("mix", SEQ, None),
        P("mix", SEQ, None),
        P(None, "mix"),
        P(None, "mix"),
        P(),
        P(None, "mix"),
        P(),
        P("mix"),
        P("mix"),
        P("mix", None),
    )
    return jax.shard_map(
        body, mesh=finer, in_specs=placed, out_specs=P("mix", SEQ, None), check_vma=False
    )
```

```python
import jax
import jax.numpy as jnp
from jax import lax
from jax.experimental import pallas as pl
from jax.experimental.pallas import tpu as pltpu
from jax.sharding import Mesh
from jax.sharding import PartitionSpec as P


F32, BF16 = jnp.float32, jnp.bfloat16
CHIPS = ("seq_0", "seq_1")
SEQ = ("seq_0", "seq_1", "seq_2")
STATE = 64
CONV = 4
BLOCK = 128
LANES = 128
HALO = 16
SHARDS = 4
PART = 16


def dot(a, b):
    return jnp.dot(a, b, preferred_element_type=F32)


def iota(shape, axis):
    return lax.broadcasted_iota(jnp.int32, shape, axis)


def ones_where(mask):
    return jnp.where(mask, 1.0, 0.0).astype(BF16)


def hi_lo(value):
    high = value.astype(BF16)
    low = (value - high.astype(F32)).astype(BF16)
    return jnp.concatenate([high, low], axis=-1)


def lower_ones(size):
    return ones_where(iota((size, size), 0) >= iota((size, size), 1))


def spread(start, width):
    shape = (2 * LANES, width)
    return ones_where((iota(shape, 0) & (LANES - 1)) == ((iota(shape, 1) + start) >> 6))


def scale_of(rate):
    z = 2.0 * rate
    series = z * (
        1.0
        + z * (1 / 2 + z * (1 / 6 + z * (1 / 24 + z * (1 / 120 + z * (1 / 720)))))
    )
    return jnp.sqrt(jnp.maximum(-jnp.where(z > -0.25, series, jnp.exp(z) - 1.0), 0.0))


def silu(value):
    return value * jax.nn.sigmoid(value)


def conv_silu(halo_rows, rows, taps):
    rows = jnp.concatenate([halo_rows, rows], axis=0).astype(BF16).astype(F32)
    total = taps[CONV - 1 : CONV] * rows
    for back in range(1, CONV):
        total = total + taps[CONV - 1 - back : CONV - back] * pltpu.roll(rows, back, 0)
    return silu(total[HALO:]).astype(BF16)


def shard_states(weight, taps, r, at, tok_ref, halo_ref, tail_ref, bt_ref, xa_ref, msg_ref):
    wide = weight.shape[1]
    xa = conv_silu(dot(halo_ref[...], weight), dot(tok_ref[...], weight), taps)
    xa_ref[:, at : at + wide] = xa
    tail = dot(tail_ref[...], spread(r * wide, wide))
    state = dot(bt_ref[0:STATE, :], (xa.astype(F32) * tail).astype(BF16)).astype(BF16)
    for p in range(wide // LANES):
        for q in range(STATE // PART):
            at_piece = (r * (wide // LANES) + p) * (STATE // PART) + q
            msg_ref[at_piece, 0:PART] = state[q * PART : (q + 1) * PART, p * LANES : (p + 1) * LANES]


def decay_kernel(c_ref, x_ref, tokens_ref, log_ref, got_ref, got_log_ref, tok_ref, edge_ref, logp_ref, tail_ref, extra_ref):
    core, mine = c_ref[0], x_ref[0]
    heads, length = log_ref.shape[1:]
    here = pl.multiple_of(core * length, length)
    there = pl.multiple_of((1 - core) * length, length)
    tok_ref[pl.ds(here, length)] = tokens_ref[core]
    tok_ref[pl.ds(there, length)] = got_ref[core]
    edge_ref[...] = tok_ref[2 * length - HALO :]
    per = heads // SHARDS
    shape = (LANES, heads)
    rel = iota(shape, 0)
    source = per * ((mine - rel // per + SHARDS) & (SHARDS - 1)) + rel % per
    order = ones_where((iota(shape, 1) == source) & (rel < heads))
    a, b = log_ref[core], got_log_ref[core]
    logs = jnp.concatenate([jnp.where(core == 0, a, b), jnp.where(core == 0, b, a)], axis=1)
    rate = dot(order, logs).T
    logp = rate.astype(BF16)
    logp_ref[...] = logp
    cum = dot(lower_ones(2 * length), logp)
    total = cum[2 * length - 1 :]
    tail_ref[...] = hi_lo(jnp.exp(total - cum) * scale_of(rate))
    width = extra_ref.shape[1]
    total_x = dot(hi_lo(jnp.broadcast_to(total, (8, LANES))), spread(0, width))
    high = total_x.astype(BF16).astype(F32)
    row = iota((8, width), 0)
    extra_ref[...] = jnp.where(row == 0, high, jnp.where(row == 1, total_x - high, 0.0)).astype(BF16)


def own_kernel(
    tok_ref, halo_ref, tail_ref, extra_ref, wbc_ref, cbc_ref, w_ref, cx_ref,
    bc_ref, bt_ref, xa_ref, msg_ref,
):
    extra = extra_ref[...]
    parts = STATE // PART
    for j in range(extra.shape[1] // LANES):
        for q in range(parts):
            msg_ref[j * parts + q, PART : PART + 8] = extra[:, j * LANES : (j + 1) * LANES]
    taps = cbc_ref[...].astype(F32)
    bc = conv_silu(dot(halo_ref[...], wbc_ref[...]), dot(tok_ref[...], wbc_ref[...]), taps)
    bc_ref[...] = bc
    bt_ref[...] = bc.astype(F32).T.astype(BF16)
    shard_states(w_ref[...], cx_ref[...].astype(F32), 0, 0, tok_ref, halo_ref, tail_ref, bt_ref, xa_ref, msg_ref)


def others_kernel(c_ref, tok_ref, halo_ref, tail_ref, bt_ref, bc_ref, logp_ref, own_msg_ref, *rest):
    here, there = rest[0 : SHARDS - 1], rest[SHARDS - 1 : 2 * SHARDS - 2]
    xa_ref, msg_ref, seen_ref, w_ref = rest[2 * SHARDS - 2 :]
    core = c_ref[0]
    seen_ref[:, 0:LANES] = bc_ref[...]
    seen_ref[:, LANES:] = logp_ref[...]
    half, wide = w_ref.shape[0] // 2, w_ref.shape[1]
    msg_ref[...] = own_msg_ref[...]
    for r in range(1, SHARDS):
        a, b = here[r - 1][0:half], there[r - 1][0:half]
        w_ref[0:half] = jnp.where(core == 0, a, b)
        w_ref[half : 2 * half] = jnp.where(core == 0, b, a)
        taps = here[r - 1][half : half + 8].astype(F32)
        shard_states(w_ref[...], taps, r, (r - 1) * wide, tok_ref, halo_ref, tail_ref, bt_ref, xa_ref, msg_ref)


def scan_kernel(s_ref, out_ref):
    def step(k, carry):
        out_ref[k] = carry.astype(BF16)
        extra = s_ref[k, PART : PART + 8].astype(F32)
        return carry * jnp.exp(extra[0:1] + extra[1:2]) + s_ref[k, 0:PART].astype(F32)

    lax.fori_loop(0, s_ref.shape[0], step, jnp.zeros((PART, LANES), F32), unroll=8)


def intra_kernel(xa0_ref, xa1_ref, seen_ref, p0_ref, *rest):
    z_refs, y_ref = rest[:-1], rest[-1]
    length, wide = xa0_ref.shape
    depth = z_refs[0].shape[0] - 8
    blocks = length // BLOCK
    lower_block = lower_ones(BLOCK)
    keep = iota((BLOCK, BLOCK), 0) >= iota((BLOCK, BLOCK), 1)
    left = iota((BLOCK, LANES), 1) < LANES // 2
    bc = seen_ref[:, 0:LANES]
    bt = bc.astype(F32).T.astype(BF16)
    logp = seen_ref[:, LANES:]
    scale = scale_of(logp.astype(F32))
    scale_t = scale.T
    span = [slice(b * BLOCK, (b + 1) * BLOCK) for b in range(blocks)]
    cums = [dot(lower_block, logp[span[b]]) for b in range(blocks)]
    cums_t = [cum.T for cum in cums]
    reads = [bc[span[b]][:, STATE:] for b in range(blocks)]
    writes_t = [bt[0:STATE, b * BLOCK : (b + 1) * BLOCK] for b in range(blocks)]
    scores = [jnp.where(keep, dot(reads[b], writes_t[b]), 0.0) for b in range(blocks)]
    enter = [hi_lo(jnp.exp(cum)) for cum in cums]
    leave = [hi_lo(jnp.exp(cums[b][BLOCK - 1 :] - cums[b]) * scale[span[b]]) for b in range(blocks)]
    last = [hi_lo(jnp.broadcast_to(jnp.exp(cums[b][BLOCK - 1 :]), (8, LANES))) for b in range(blocks)]
    for j in range(SHARDS * wide // LANES):
        lanes = slice(j * LANES, (j + 1) * LANES)
        to_lanes = spread(j * LANES, LANES)
        r, at = divmod(j * LANES, wide)
        extra = p0_ref[...] if r == 0 else z_refs[r - 1][depth : depth + 8]
        skip = extra[1:2, at : at + LANES].astype(F32)
        state = None
        for b in range(blocks):
            if j * LANES < wide:
                xb = xa0_ref[span[b], lanes]
            else:
                xb = xa1_ref[span[b], j * LANES - wide : (j + 1) * LANES - wide]
            parts = []
            for h in (2 * j, 2 * j + 1):
                seg = cums[b][:, h : h + 1] - cums_t[b][h : h + 1, :]
                decay = jnp.exp(jnp.minimum(seg, 0.0))
                weights = decay * (scores[b] * scale_t[h : h + 1, span[b]])
                parts.append(weights.astype(BF16))
            zero = jnp.zeros_like(xb)
            split = jnp.concatenate([jnp.where(left, xb, zero), jnp.where(left, zero, xb)], axis=0)
            y = dot(jnp.concatenate(parts, axis=1), split) + skip * xb.astype(F32)
            if state is not None:
                y = y + dot(enter[b], to_lanes) * dot(reads[b], state.astype(BF16))
            if b + 1 < blocks:
                scaled = (xb.astype(F32) * dot(leave[b], to_lanes)).astype(BF16)
                fresh = dot(writes_t[b], scaled)
                state = fresh if state is None else fresh + dot(last[b], to_lanes)[0:1] * state
            y_ref[span[b], lanes] = y.astype(BF16)


def gate_kernel(c_ref, tok_ref, seen_ref, y_ref, wz0_ref, wo0_ref, p0_ref, *rest):
    here, there = rest[0 : SHARDS - 1], rest[SHARDS - 1 : 2 * SHARDS - 2]
    yg_ref, eg_ref, wo_ref, gain_ref, wz_ref = rest[2 * SHARDS - 2 :]
    core = c_ref[0]
    depth, wide = wz0_ref.shape
    half, q = depth // 2, wide // 2
    length = tok_ref.shape[0]
    wo_ref[0:wide] = wo0_ref[...]
    grow = hi_lo(jnp.exp(dot(lower_ones(length), seen_ref[:, LANES:])))
    for r in range(SHARDS):
        if r == 0:
            wz_ref[...] = wz0_ref[...]
            extra = p0_ref[...]
        else:
            a, b = here[r - 1], there[r - 1]
            wz_ref[0:half] = jnp.where(core == 0, a[0:half], b[0:half])
            wz_ref[half:depth] = jnp.where(core == 0, b[0:half], a[0:half])
            for s in range(2):
                part = slice(half + s * q, half + (s + 1) * q)
                lanes = slice(s * wide, (s + 1) * wide)
                wo_ref[r * wide : r * wide + q, lanes] = jnp.where(core == 0, a[part], b[part])
                wo_ref[r * wide + q : (r + 1) * wide, lanes] = jnp.where(core == 0, b[part], a[part])
            extra = a[2 * half : 2 * half + 8]
        lanes = slice(r * wide, (r + 1) * wide)
        gain_ref[:, lanes] = extra
        gate = silu(dot(tok_ref[...], wz_ref[...]).astype(BF16).astype(F32))
        yg_ref[:, lanes] = (y_ref[:, lanes].astype(F32) * gate).astype(BF16)
        eg_ref[:, lanes] = (dot(grow, spread(r * wide, wide)) * gate).astype(BF16)


def final_rows(start, back_ref, seen_ref, yg_ref, eg_ref, gain_ref, wo_ref, normed_ref):
    length, width = normed_ref.shape
    rows = pl.ds(pl.multiple_of(start, length), length)
    read = seen_ref[rows, STATE : 2 * STATE]
    shape = (2 * LANES, LANES)
    same_head = ones_where(((iota(shape, 0) & (LANES - 1)) >> 6) == (iota(shape, 1) >> 6))
    parts = STATE // PART
    for j in range(width // LANES):
        lanes = slice(j * LANES, (j + 1) * LANES)
        carry = jnp.concatenate([back_ref[j * parts + q] for q in range(parts)], axis=0)
        v = yg_ref[rows, lanes].astype(F32) + eg_ref[rows, lanes].astype(F32) * dot(read, carry)
        mean = dot(hi_lo(v * v), same_head) * (1.0 / 64.0)
        gain = gain_ref[0:1, lanes].astype(F32)
        normed_ref[:, lanes] = (v * lax.rsqrt(mean + 1e-05) * gain).astype(BF16)
    return dot(normed_ref[...], wo_ref[...]).astype(BF16)


def final_send_kernel(c_ref, back_ref, seen_ref, yg_ref, eg_ref, gain_ref, wo_ref, out_ref, normed_ref):
    start = (1 - c_ref[0]) * normed_ref.shape[0]
    out_ref[...] = final_rows(start, back_ref, seen_ref, yg_ref, eg_ref, gain_ref, wo_ref, normed_ref)


def final_own_kernel(c_ref, back_ref, seen_ref, yg_ref, eg_ref, gain_ref, wo_ref, out_ref, normed_ref):
    start = c_ref[0] * normed_ref.shape[0]
    out_ref[...] = final_rows(start, back_ref, seen_ref, yg_ref, eg_ref, gain_ref, wo_ref, normed_ref)


def join_kernel(c_ref, own_ref, got_ref, out_ref, sems):
    core = c_ref[0]
    copies = [
        pltpu.make_async_copy(own_ref, out_ref.at[core], sems.at[0]),
        pltpu.make_async_copy(got_ref, out_ref.at[1 - core], sems.at[1]),
    ]
    for copy in copies:
        copy.start()
    for copy in copies:
        copy.wait()


VMEM = pl.BlockSpec(memory_space=pltpu.VMEM)
SMEM = pl.BlockSpec(memory_space=pltpu.SMEM)
HBM = pl.BlockSpec(memory_space=pltpu.HBM)
ANY = pl.BlockSpec()


def call(kernel, outs, args, specs, out_specs=None, scratch=(), flops=0, mib=24):
    return pl.pallas_call(
        kernel,
        out_shape=[jax.ShapeDtypeStruct(shape, dtype) for shape, dtype in outs],
        in_specs=specs,
        out_specs=out_specs or [VMEM] * len(outs),
        scratch_shapes=list(scratch),
        compiler_params=pltpu.CompilerParams(vmem_limit_bytes=mib * 2**20),
        cost_estimate=pl.CostEstimate(flops=flops, bytes_accessed=2**20, transcendentals=0),
    )(*args)


def around(value, axis, steps):
    count = lax.axis_size(axis)
    return lax.ppermute(value, axis, [(k, (k + steps) % count) for k in range(count)])


def padded(value, above, rows, columns=None):
    columns = value.shape[1] if columns is None else columns
    return lax.pad(
        value, jnp.zeros((), value.dtype), [(above, rows - above - value.shape[0], 0), (0, columns - value.shape[1], 0)]
    )


def layer(tokens, log_forget_rate, w_x, w_z, w_bc, conv_x, conv_bc, skip, gain, w_out):
    core, across = lax.axis_index("seq_2"), lax.axis_index("mix")
    core_s, across_s = core.astype(jnp.int32)[None], across.astype(jnp.int32)[None]
    _, length, depth = tokens.shape
    wide = w_x.shape[1]
    width = wide * SHARDS
    half = depth // 2
    chips = lax.axis_size(CHIPS)
    both = 2 * length
    logs = jnp.swapaxes(log_forget_rate, 1, 2)
    parts = width // LANES * (STATE // PART)

    low = core == 0
    first = padded(jnp.where(low, w_x[:half], w_x[half:]), 0, half + 8) + padded(conv_x, half, half + 8)
    x_here = [around(first, "mix", r) for r in (2, 1, 3)]
    x_here = [x_here[1], x_here[0], x_here[2]]
    got = around(tokens, "seq_2", 1)
    got_log = around(logs, "seq_2", 1)
    tok, edge, logp, tail, extra = call(
        decay_kernel,
        [
            ((both, depth), BF16),
            ((HALO, depth), BF16),
            ((both, LANES), BF16),
            ((both, 2 * LANES), BF16),
            ((8, width), BF16),
        ],
        (core_s, across_s, tokens, logs, got, got_log),
        [SMEM, SMEM, ANY, ANY, VMEM, VMEM],
        flops=10**9,
    )
    halo = lax.ppermute(edge, CHIPS, [(k, k + 1) for k in range(chips - 1)])
    bc, bt, xa0, own_msg = call(
        own_kernel,
        [((both, 2 * STATE), BF16), ((2 * STATE, both), BF16), ((both, wide), BF16), ((parts, PART + 8, LANES), BF16)],
        (tok, halo, tail, extra, w_bc, conv_bc, w_x, conv_x),
        [VMEM] * 4 + [ANY] * 4,
        flops=10**9,
    )
    w_z, w_out, gain, skip, tok = lax.optimization_barrier((w_z, w_out, gain, skip, tok))
    p0 = padded(gain[None], 0, 8) + padded(jnp.repeat(skip, wide // skip.shape[0])[None], 1, 8)
    out_half = jnp.where(low, w_out[: wide // 2], w_out[wide // 2 :])
    rows = 2 * half + 8
    second = (
        padded(jnp.where(low, w_z[:half], w_z[half:]), 0, rows)
        + padded(out_half[:, :wide], half, rows)
        + padded(out_half[:, wide:], half + wide // 2, rows)
        + padded(p0, 2 * half, rows)
    )
    z_here = [around(second, "mix", r) for r in range(1, SHARDS)]

    (x_here, own_msg) = lax.optimization_barrier((x_here, own_msg))
    x_there = [around(part, "seq_2", 1) for part in x_here]
    xa1, msg, seen = call(
        others_kernel,
        [((both, width - wide), BF16), ((parts, PART + 8, LANES), BF16), ((both, 2 * LANES), BF16)],
        (core_s, tok, halo, tail, bt, bc, logp, own_msg, *x_here, *x_there),
        [SMEM] + [VMEM] * 13,
        scratch=[pltpu.VMEM((depth, wide), BF16)],
        flops=10**9,
    )
    arrived = lax.all_to_all(msg, CHIPS, 0, 0)
    (y,) = call(intra_kernel, [((both, width), BF16)], (xa0, xa1, seen, p0, *z_here), [VMEM] * 7, flops=2 * 10**9)
    (carries,) = call(scan_kernel, [((parts, PART, LANES), BF16)], (arrived,), [VMEM], flops=10**7)
    z_there = [around(part, "seq_2", 1) for part in z_here]
    back = lax.all_to_all(carries, CHIPS, 0, 0)
    y, back = lax.optimization_barrier((y, back))
    yg, eg, wo, gains = call(
        gate_kernel,
        [((both, width), BF16), ((both, width), BF16), ((width, depth), BF16), ((8, width), BF16)],
        (core_s, tok, seen, y, w_z, w_out, p0, *z_here, *z_there),
        [SMEM] + [ANY] * 12,
        scratch=[pltpu.VMEM((depth, wide), BF16)],
        flops=2 * 10**9,
    )
    ends = (core_s, back, seen, yg, eg, gains, wo)
    specs = [SMEM, VMEM, ANY, VMEM, VMEM, VMEM, VMEM]
    scratch = [pltpu.VMEM((length, width), BF16)]
    (away,) = call(final_send_kernel, [((length, depth), BF16)], ends, specs, scratch=scratch, flops=10**9)
    back_home = around(away, "seq_2", 1)
    (home,) = call(final_own_kernel, [((length, depth), BF16)], ends, specs, scratch=scratch, flops=10**9)
    (mixed,) = call(
        join_kernel,
        [((2, length, depth), BF16)],
        (core_s, home, back_home),
        [SMEM, VMEM, VMEM],
        out_specs=[HBM],
        scratch=[pltpu.SemaphoreType.DMA((2,))],
    )
    return mixed


def solution(mesh):
    finer = Mesh(
        mesh.devices.reshape(8, 4, 2, mesh.shape["mix"]), ("seq_0", "seq_1", "seq_2", "mix")
    )
    placed = (
        P("mix", SEQ, None),
        P("mix", SEQ, None),
        P(None, "mix"),
        P(None, "mix"),
        P(),
        P(None, "mix"),
        P(),
        P("mix"),
        P("mix"),
        P("mix", None),
    )
    return jax.shard_map(layer, mesh=finer, in_specs=placed, out_specs=P("mix", SEQ, None), check_vma=False)
```

```python
import jax
import jax.numpy as jnp
from jax import lax
from jax.experimental import pallas as pl
from jax.experimental.pallas import tpu as pltpu
from jax.sharding import Mesh
from jax.sharding import PartitionSpec as P


F32, BF16 = jnp.float32, jnp.bfloat16
CHIPS = ("seq_0", "seq_1")
SEQ = ("seq_0", "seq_1", "seq_2")
STATE = 64
CONV = 4
BLOCK = 128
LANES = 128
HALO = 16
SHARDS = 4
PART = 16


def dot(a, b):
    return jnp.dot(a, b, preferred_element_type=F32)


def iota(shape, axis):
    return lax.broadcasted_iota(jnp.int32, shape, axis)


def ones_where(mask):
    return jnp.where(mask, 1.0, 0.0).astype(BF16)


def hi_lo(value):
    high = value.astype(BF16)
    low = (value - high.astype(F32)).astype(BF16)
    return jnp.concatenate([high, low], axis=-1)


def lower_ones(size):
    return ones_where(iota((size, size), 0) >= iota((size, size), 1))


def spread(start, width):
    shape = (2 * LANES, width)
    return ones_where((iota(shape, 0) & (LANES - 1)) == ((iota(shape, 1) + start) >> 6))


def scale_of(rate):
    z = 2.0 * rate
    series = z * (
        1.0
        + z * (1 / 2 + z * (1 / 6 + z * (1 / 24 + z * (1 / 120 + z * (1 / 720)))))
    )
    return jnp.sqrt(jnp.maximum(-jnp.where(z > -0.25, series, jnp.exp(z) - 1.0), 0.0))


def silu(value):
    return value * jax.nn.sigmoid(value)


def conv_silu(halo_rows, rows, taps):
    rows = jnp.concatenate([halo_rows, rows], axis=0).astype(BF16).astype(F32)
    total = taps[CONV - 1 : CONV] * rows
    for back in range(1, CONV):
        total = total + taps[CONV - 1 - back : CONV - back] * pltpu.roll(rows, back, 0)
    return silu(total[HALO:]).astype(BF16)


def shard_states(weight, taps, r, at, tok_ref, halo_ref, tail_ref, bt_ref, xa_ref, msg_ref):
    wide = weight.shape[1]
    xa = conv_silu(dot(halo_ref[...], weight), dot(tok_ref[...], weight), taps)
    xa_ref[:, at : at + wide] = xa
    tail = dot(tail_ref[...], spread(r * wide, wide))
    state = dot(bt_ref[0:STATE, :], (xa.astype(F32) * tail).astype(BF16)).astype(BF16)
    for p in range(wide // LANES):
        for q in range(STATE // PART):
            at_piece = (r * (wide // LANES) + p) * (STATE // PART) + q
            msg_ref[at_piece, 0:PART] = state[q * PART : (q + 1) * PART, p * LANES : (p + 1) * LANES]


def decay_kernel(c_ref, x_ref, tokens_ref, log_ref, got_ref, got_log_ref, tok_ref, edge_ref, logp_ref, tail_ref, extra_ref):
    core, mine = c_ref[0], x_ref[0]
    heads, length = log_ref.shape[1:]
    here = pl.multiple_of(core * length, length)
    there = pl.multiple_of((1 - core) * length, length)
    tok_ref[pl.ds(here, length)] = tokens_ref[core]
    tok_ref[pl.ds(there, length)] = got_ref[core]
    edge_ref[...] = tok_ref[2 * length - HALO :]
    per = heads // SHARDS
    shape = (LANES, heads)
    rel = iota(shape, 0)
    source = per * ((mine - rel // per + SHARDS) & (SHARDS - 1)) + rel % per
    order = ones_where((iota(shape, 1) == source) & (rel < heads))
    a, b = log_ref[core], got_log_ref[core]
    logs = jnp.concatenate([jnp.where(core == 0, a, b), jnp.where(core == 0, b, a)], axis=1)
    rate = dot(order, logs).T
    logp = rate.astype(BF16)
    logp_ref[...] = logp
    cum = dot(lower_ones(2 * length), logp)
    total = cum[2 * length - 1 :]
    tail_ref[...] = hi_lo(jnp.exp(total - cum) * scale_of(rate))
    width = extra_ref.shape[1]
    total_x = dot(hi_lo(jnp.broadcast_to(total, (8, LANES))), spread(0, width))
    high = total_x.astype(BF16).astype(F32)
    row = iota((8, width), 0)
    extra_ref[...] = jnp.where(row == 0, high, jnp.where(row == 1, total_x - high, 0.0)).astype(BF16)


def own_kernel(
    tok_ref, halo_ref, tail_ref, extra_ref, wbc_ref, cbc_ref, w_ref, cx_ref,
    bc_ref, bt_ref, xa_ref, msg_ref,
):
    extra = extra_ref[...]
    parts = STATE // PART
    for j in range(extra.shape[1] // LANES):
        for q in range(parts):
            msg_ref[j * parts + q, PART : PART + 8] = extra[:, j * LANES : (j + 1) * LANES]
    taps = cbc_ref[...].astype(F32)
    bc = conv_silu(dot(halo_ref[...], wbc_ref[...]), dot(tok_ref[...], wbc_ref[...]), taps)
    bc_ref[...] = bc
    bt_ref[...] = bc.astype(F32).T.astype(BF16)
    shard_states(w_ref[...], cx_ref[...].astype(F32), 0, 0, tok_ref, halo_ref, tail_ref, bt_ref, xa_ref, msg_ref)


def others_kernel(c_ref, tok_ref, halo_ref, tail_ref, bt_ref, bc_ref, logp_ref, own_msg_ref, own_prm_ref, *rest):
    here, there = rest[0 : SHARDS - 1], rest[SHARDS - 1 : 2 * SHARDS - 2]
    xa_ref, msg_ref, seen_ref, prm_ref, w_ref = rest[2 * SHARDS - 2 :]
    core = c_ref[0]
    seen_ref[:, 0:LANES] = bc_ref[...]
    seen_ref[:, LANES:] = logp_ref[...]
    half, wide = w_ref.shape[0] // 2, w_ref.shape[1]
    msg_ref[...] = own_msg_ref[...]
    prm_ref[:, 0:wide] = own_prm_ref[...]
    for r in range(1, SHARDS):
        a, b = here[r - 1][0:half], there[r - 1][0:half]
        w_ref[0:half] = jnp.where(core == 0, a, b)
        w_ref[half : 2 * half] = jnp.where(core == 0, b, a)
        prm_ref[:, r * wide : (r + 1) * wide] = here[r - 1][half : half + 8]
        taps = here[r - 1][half : half + 8].astype(F32)
        shard_states(w_ref[...], taps, r, (r - 1) * wide, tok_ref, halo_ref, tail_ref, bt_ref, xa_ref, msg_ref)


def scan_kernel(s_ref, out_ref):
    def step(k, carry):
        out_ref[k] = carry.astype(BF16)
        extra = s_ref[k, PART : PART + 8].astype(F32)
        return carry * jnp.exp(extra[0:1] + extra[1:2]) + s_ref[k, 0:PART].astype(F32)

    lax.fori_loop(0, s_ref.shape[0], step, jnp.zeros((PART, LANES), F32), unroll=8)


def intra_kernel(xa0_ref, xa1_ref, seen_ref, prm_ref, y_ref):
    length, wide = xa0_ref.shape
    blocks = length // BLOCK
    lower_block = lower_ones(BLOCK)
    keep = iota((BLOCK, BLOCK), 0) >= iota((BLOCK, BLOCK), 1)
    left = iota((BLOCK, LANES), 1) < LANES // 2
    bc = seen_ref[:, 0:LANES]
    bt = bc.astype(F32).T.astype(BF16)
    logp = seen_ref[:, LANES:]
    scale = scale_of(logp.astype(F32))
    scale_t = scale.T
    span = [slice(b * BLOCK, (b + 1) * BLOCK) for b in range(blocks)]
    cums = [dot(lower_block, logp[span[b]]) for b in range(blocks)]
    cums_t = [cum.T for cum in cums]
    reads = [bc[span[b]][:, STATE:] for b in range(blocks)]
    writes_t = [bt[0:STATE, b * BLOCK : (b + 1) * BLOCK] for b in range(blocks)]
    scores = [jnp.where(keep, dot(reads[b], writes_t[b]), 0.0) for b in range(blocks)]
    enter = [hi_lo(jnp.exp(cum)) for cum in cums]
    leave = [hi_lo(jnp.exp(cums[b][BLOCK - 1 :] - cums[b]) * scale[span[b]]) for b in range(blocks)]
    last = [hi_lo(jnp.broadcast_to(jnp.exp(cums[b][BLOCK - 1 :]), (8, LANES))) for b in range(blocks)]
    for j in range(SHARDS * wide // LANES):
        lanes = slice(j * LANES, (j + 1) * LANES)
        to_lanes = spread(j * LANES, LANES)
        skip = prm_ref[CONV + 1 : CONV + 2, lanes].astype(F32)
        state = None
        for b in range(blocks):
            if j * LANES < wide:
                xb = xa0_ref[span[b], lanes]
            else:
                xb = xa1_ref[span[b], j * LANES - wide : (j + 1) * LANES - wide]
            parts = []
            for h in (2 * j, 2 * j + 1):
                seg = cums[b][:, h : h + 1] - cums_t[b][h : h + 1, :]
                decay = jnp.exp(jnp.minimum(seg, 0.0))
                weights = decay * (scores[b] * scale_t[h : h + 1, span[b]])
                parts.append(weights.astype(BF16))
            zero = jnp.zeros_like(xb)
            split = jnp.concatenate([jnp.where(left, xb, zero), jnp.where(left, zero, xb)], axis=0)
            y = dot(jnp.concatenate(parts, axis=1), split) + skip * xb.astype(F32)
            if state is not None:
                y = y + dot(enter[b], to_lanes) * dot(reads[b], state.astype(BF16))
            if b + 1 < blocks:
                scaled = (xb.astype(F32) * dot(leave[b], to_lanes)).astype(BF16)
                fresh = dot(writes_t[b], scaled)
                state = fresh if state is None else fresh + dot(last[b], to_lanes)[0:1] * state
            y_ref[span[b], lanes] = y.astype(BF16)


def gate_kernel(c_ref, tok_ref, seen_ref, y_ref, wz0_ref, wo0_ref, *rest):
    here, there = rest[0 : SHARDS - 1], rest[SHARDS - 1 : 2 * SHARDS - 2]
    yg_ref, eg_ref, wo_ref, wz_ref = rest[2 * SHARDS - 2 :]
    core = c_ref[0]
    depth, wide = wz0_ref.shape
    half, q = depth // 2, wide // 2
    length = tok_ref.shape[0]
    wo_ref[0:wide] = wo0_ref[...]
    grow = hi_lo(jnp.exp(dot(lower_ones(length), seen_ref[:, LANES:])))
    for r in range(SHARDS):
        if r == 0:
            wz_ref[...] = wz0_ref[...]
        else:
            a, b = here[r - 1], there[r - 1]
            wz_ref[0:half] = jnp.where(core == 0, a[0:half], b[0:half])
            wz_ref[half:depth] = jnp.where(core == 0, b[0:half], a[0:half])
            for s in range(2):
                part = slice(half + s * q, half + (s + 1) * q)
                lanes = slice(s * wide, (s + 1) * wide)
                wo_ref[r * wide : r * wide + q, lanes] = jnp.where(core == 0, a[part], b[part])
                wo_ref[r * wide + q : (r + 1) * wide, lanes] = jnp.where(core == 0, b[part], a[part])
        lanes = slice(r * wide, (r + 1) * wide)
        gate = silu(dot(tok_ref[...], wz_ref[...]).astype(BF16).astype(F32))
        yg_ref[:, lanes] = (y_ref[:, lanes].astype(F32) * gate).astype(BF16)
        eg_ref[:, lanes] = (dot(grow, spread(r * wide, wide)) * gate).astype(BF16)


def final_rows(start, back_ref, seen_ref, yg_ref, eg_ref, gain_ref, wo_ref, normed_ref):
    length, width = normed_ref.shape
    rows = pl.ds(pl.multiple_of(start, length), length)
    read = seen_ref[rows, STATE : 2 * STATE]
    shape = (2 * LANES, LANES)
    same_head = ones_where(((iota(shape, 0) & (LANES - 1)) >> 6) == (iota(shape, 1) >> 6))
    parts = STATE // PART
    for j in range(width // LANES):
        lanes = slice(j * LANES, (j + 1) * LANES)
        carry = jnp.concatenate([back_ref[j * parts + q] for q in range(parts)], axis=0)
        v = yg_ref[rows, lanes].astype(F32) + eg_ref[rows, lanes].astype(F32) * dot(read, carry)
        mean = dot(hi_lo(v * v), same_head) * (1.0 / 64.0)
        gain = gain_ref[CONV : CONV + 1, lanes].astype(F32)
        normed_ref[:, lanes] = (v * lax.rsqrt(mean + 1e-05) * gain).astype(BF16)
    return dot(normed_ref[...], wo_ref[...]).astype(BF16)


def final_send_kernel(c_ref, back_ref, seen_ref, yg_ref, eg_ref, gain_ref, wo_ref, out_ref, normed_ref):
    start = (1 - c_ref[0]) * normed_ref.shape[0]
    out_ref[...] = final_rows(start, back_ref, seen_ref, yg_ref, eg_ref, gain_ref, wo_ref, normed_ref)


def final_own_kernel(c_ref, back_ref, seen_ref, yg_ref, eg_ref, gain_ref, wo_ref, out_ref, normed_ref):
    start = c_ref[0] * normed_ref.shape[0]
    out_ref[...] = final_rows(start, back_ref, seen_ref, yg_ref, eg_ref, gain_ref, wo_ref, normed_ref)


def join_kernel(c_ref, own_ref, got_ref, out_ref, sems):
    core = c_ref[0]
    copies = [
        pltpu.make_async_copy(own_ref, out_ref.at[core], sems.at[0]),
        pltpu.make_async_copy(got_ref, out_ref.at[1 - core], sems.at[1]),
    ]
    for copy in copies:
        copy.start()
    for copy in copies:
        copy.wait()


VMEM = pl.BlockSpec(memory_space=pltpu.VMEM)
SMEM = pl.BlockSpec(memory_space=pltpu.SMEM)
HBM = pl.BlockSpec(memory_space=pltpu.HBM)
ANY = pl.BlockSpec()


def call(kernel, outs, args, specs, out_specs=None, scratch=(), flops=0, mib=24):
    return pl.pallas_call(
        kernel,
        out_shape=[jax.ShapeDtypeStruct(shape, dtype) for shape, dtype in outs],
        in_specs=specs,
        out_specs=out_specs or [VMEM] * len(outs),
        scratch_shapes=list(scratch),
        compiler_params=pltpu.CompilerParams(vmem_limit_bytes=mib * 2**20),
        cost_estimate=pl.CostEstimate(flops=flops, bytes_accessed=2**20, transcendentals=0),
    )(*args)


def around(value, axis, steps):
    count = lax.axis_size(axis)
    return lax.ppermute(value, axis, [(k, (k + steps) % count) for k in range(count)])


def padded(value, above, rows, columns=None):
    columns = value.shape[1] if columns is None else columns
    return lax.pad(
        value, jnp.zeros((), value.dtype), [(above, rows - above - value.shape[0], 0), (0, columns - value.shape[1], 0)]
    )


def layer(tokens, log_forget_rate, w_x, w_z, w_bc, conv_x, conv_bc, skip, gain, w_out):
    core, across = lax.axis_index("seq_2"), lax.axis_index("mix")
    core_s, across_s = core.astype(jnp.int32)[None], across.astype(jnp.int32)[None]
    _, length, depth = tokens.shape
    wide = w_x.shape[1]
    width = wide * SHARDS
    half = depth // 2
    chips = lax.axis_size(CHIPS)
    both = 2 * length
    logs = jnp.swapaxes(log_forget_rate, 1, 2)
    parts = width // LANES * (STATE // PART)

    low = core == 0
    extra = (
        padded(conv_x, 0, 8) + padded(gain[None], CONV, 8) + padded(jnp.repeat(skip, wide // skip.shape[0])[None], CONV + 1, 8)
    )
    first = padded(jnp.where(low, w_x[:half], w_x[half:]), 0, half + 8) + padded(extra, half, half + 8)
    x_here = [around(first, "mix", r) for r in (2, 1, 3)]
    x_here = [x_here[1], x_here[0], x_here[2]]
    got = around(tokens, "seq_2", 1)
    got_log = around(logs, "seq_2", 1)
    tok, edge, logp, tail, totals = call(
        decay_kernel,
        [
            ((both, depth), BF16),
            ((HALO, depth), BF16),
            ((both, LANES), BF16),
            ((both, 2 * LANES), BF16),
            ((8, width), BF16),
        ],
        (core_s, across_s, tokens, logs, got, got_log),
        [SMEM, SMEM, ANY, ANY, VMEM, VMEM],
        flops=10**9,
    )
    halo = lax.ppermute(edge, CHIPS, [(k, k + 1) for k in range(chips - 1)])
    bc, bt, xa0, own_msg = call(
        own_kernel,
        [((both, 2 * STATE), BF16), ((2 * STATE, both), BF16), ((both, wide), BF16), ((parts, PART + 8, LANES), BF16)],
        (tok, halo, tail, totals, w_bc, conv_bc, w_x, conv_x),
        [VMEM] * 4 + [ANY] * 4,
        flops=10**9,
    )
    x_there = [around(part, "seq_2", 1) for part in x_here]
    xa1, msg, seen, prm = call(
        others_kernel,
        [((both, width - wide), BF16), ((parts, PART + 8, LANES), BF16), ((both, 2 * LANES), BF16), ((8, width), BF16)],
        (core_s, tok, halo, tail, bt, bc, logp, own_msg, extra, *x_here, *x_there),
        [SMEM] + [VMEM] * 14,
        scratch=[pltpu.VMEM((depth, wide), BF16)],
        flops=10**9,
    )
    arrived = lax.all_to_all(msg, CHIPS, 0, 0)
    w_z, w_out, _ = lax.optimization_barrier((w_z, w_out, msg))
    out_half = jnp.where(low, w_out[: wide // 2], w_out[wide // 2 :])
    second = (
        padded(jnp.where(low, w_z[:half], w_z[half:]), 0, depth)
        + padded(out_half[:, :wide], half, depth)
        + padded(out_half[:, wide:], half + wide // 2, depth)
    )
    z_here = [around(second, "mix", r) for r in (2, 1, 3)]
    z_here = [z_here[1], z_here[0], z_here[2]]
    (carries,) = call(scan_kernel, [((parts, PART, LANES), BF16)], (arrived,), [VMEM], flops=10**7)
    back = lax.all_to_all(carries, CHIPS, 0, 0)
    (y,) = call(intra_kernel, [((both, width), BF16)], (xa0, xa1, seen, prm), [VMEM] * 4, flops=2 * 10**9)
    z_here, y = lax.optimization_barrier((z_here, y))
    z_there = [around(part, "seq_2", 1) for part in z_here]
    y, back = lax.optimization_barrier((y, back))
    yg, eg, wo = call(
        gate_kernel,
        [((both, width), BF16), ((both, width), BF16), ((width, depth), BF16)],
        (core_s, tok, seen, y, w_z, w_out, *z_here, *z_there),
        [SMEM] + [ANY] * 11,
        scratch=[pltpu.VMEM((depth, wide), BF16)],
        flops=2 * 10**9,
    )
    ends = (core_s, back, seen, yg, eg, prm, wo)
    specs = [SMEM, VMEM, ANY, VMEM, VMEM, VMEM, VMEM]
    scratch = [pltpu.VMEM((length, width), BF16)]
    (away,) = call(final_send_kernel, [((length, depth), BF16)], ends, specs, scratch=scratch, flops=10**9)
    back_home = around(away, "seq_2", 1)
    (home,) = call(final_own_kernel, [((length, depth), BF16)], ends, specs, scratch=scratch, flops=10**9)
    (mixed,) = call(
        join_kernel,
        [((2, length, depth), BF16)],
        (core_s, home, back_home),
        [SMEM, VMEM, VMEM],
        out_specs=[HBM],
        scratch=[pltpu.SemaphoreType.DMA((2,))],
    )
    return mixed


def solution(mesh):
    finer = Mesh(
        mesh.devices.reshape(8, 4, 2, mesh.shape["mix"]), ("seq_0", "seq_1", "seq_2", "mix")
    )
    placed = (
        P("mix", SEQ, None),
        P("mix", SEQ, None),
        P(None, "mix"),
        P(None, "mix"),
        P(),
        P(None, "mix"),
        P(),
        P("mix"),
        P("mix"),
        P("mix", None),
    )
    return jax.shard_map(layer, mesh=finer, in_specs=placed, out_specs=P("mix", SEQ, None), check_vma=False)
```

```python
import jax
import jax.numpy as jnp
from jax import lax
from jax.experimental import pallas as pl
from jax.experimental.pallas import tpu as pltpu
from jax.sharding import Mesh
from jax.sharding import PartitionSpec as P


F32, BF16 = jnp.float32, jnp.bfloat16
CHIPS = ("seq_0", "seq_1")
SEQ = ("seq_0", "seq_1", "seq_2")
STATE = 64
CONV = 4
BLOCK = 128
LANES = 128
HALO = 16
SHARDS = 4
HEADS = 16
PART = 16


def dot(a, b):
    return jnp.dot(a, b, preferred_element_type=F32)


def iota(shape, axis):
    return lax.broadcasted_iota(jnp.int32, shape, axis)


def ones_where(mask):
    return jnp.where(mask, 1.0, 0.0).astype(BF16)


def two_terms(value):
    high = value.astype(BF16)
    low = (value - high.astype(F32)).astype(BF16)
    return jnp.concatenate([high, low], axis=-1)


def hi_lo(value):
    value = jnp.where(iota(value.shape, 1) < HEADS, value, 0.0)
    high = value.astype(BF16).astype(F32)
    return (high + pltpu.roll(value - high, HEADS, 1)).astype(BF16)


def lower_ones(size):
    return ones_where(iota((size, size), 0) >= iota((size, size), 1))


def spread(start, width):
    shape = (LANES, width)
    row = iota(shape, 0)
    return ones_where(((row & (HEADS - 1)) == ((iota(shape, 1) + start) >> 6)) & (row < 2 * HEADS))


def scale_of(rate):
    z = 2.0 * rate
    series = z * (
        1.0
        + z * (1 / 2 + z * (1 / 6 + z * (1 / 24 + z * (1 / 120 + z * (1 / 720)))))
    )
    return jnp.sqrt(jnp.maximum(-jnp.where(z > -0.25, series, jnp.exp(z) - 1.0), 0.0))


def silu(value):
    return value * jax.nn.sigmoid(value)


def conv_silu(halo_rows, rows, taps):
    rows = jnp.concatenate([halo_rows, rows], axis=0).astype(BF16).astype(F32)
    total = taps[CONV - 1 : CONV] * rows
    for back in range(1, CONV):
        total = total + taps[CONV - 1 - back : CONV - back] * pltpu.roll(rows, back, 0)
    return silu(total[HALO:]).astype(BF16)


def shard_states(weight, taps, r, at, tok_ref, halo_ref, tail_ref, bt_ref, xa_ref, msg_ref):
    wide = weight.shape[1]
    xa = conv_silu(dot(halo_ref[...], weight), dot(tok_ref[...], weight), taps)
    xa_ref[:, at : at + wide] = xa
    tail = dot(tail_ref[...], spread(r * wide, wide))
    state = dot(bt_ref[0:STATE, :], (xa.astype(F32) * tail).astype(BF16)).astype(BF16)
    for p in range(wide // LANES):
        for q in range(STATE // PART):
            at_piece = (r * (wide // LANES) + p) * (STATE // PART) + q
            msg_ref[at_piece, 0:PART] = state[q * PART : (q + 1) * PART, p * LANES : (p + 1) * LANES]


def decay_kernel(c_ref, x_ref, tokens_ref, log_ref, got_ref, got_log_ref, tok_ref, logp_ref, tail_ref, extra_ref):
    core, mine = c_ref[0], x_ref[0]
    heads, length = log_ref.shape[1:]
    here = pl.multiple_of(core * length, length)
    there = pl.multiple_of((1 - core) * length, length)
    tok_ref[pl.ds(here, length)] = tokens_ref[core]
    tok_ref[pl.ds(there, length)] = got_ref[core]
    per = heads // SHARDS
    shape = (LANES, heads)
    rel = iota(shape, 0)
    source = per * ((mine - rel // per + SHARDS) & (SHARDS - 1)) + rel % per
    order = ones_where((iota(shape, 1) == source) & (rel < heads))
    a, b = log_ref[core], got_log_ref[core]
    logs = jnp.concatenate([jnp.where(core == 0, a, b), jnp.where(core == 0, b, a)], axis=1)
    rate = dot(order, logs).T
    logp = rate.astype(BF16)
    logp_ref[...] = logp
    cum = dot(lower_ones(2 * length), logp)
    total = cum[2 * length - 1 :]
    tail_ref[...] = hi_lo(jnp.exp(total - cum) * scale_of(rate))
    width = extra_ref.shape[1]
    total_x = dot(hi_lo(jnp.broadcast_to(total, (8, LANES))), spread(0, width))
    high = total_x.astype(BF16).astype(F32)
    row = iota((8, width), 0)
    extra_ref[...] = jnp.where(row == 0, high, jnp.where(row == 1, total_x - high, 0.0)).astype(BF16)


def own_kernel(
    c_ref, tok_ref, h0_ref, h1_ref, tail_ref, extra_ref, wbc_ref, w_ref, prm_ref,
    halo_ref, bc_ref, bt_ref, xa_ref, msg_ref,
):
    core = c_ref[0]
    halo_ref[...] = h0_ref[core] + h1_ref[core]
    extra = extra_ref[...]
    parts = STATE // PART
    for j in range(extra.shape[1] // LANES):
        for q in range(parts):
            msg_ref[j * parts + q, PART : PART + 8] = extra[:, j * LANES : (j + 1) * LANES]
    prm = prm_ref[...].astype(F32)
    taps = prm[8 : 8 + CONV, 0 : 2 * STATE]
    bc = conv_silu(dot(halo_ref[...], wbc_ref[...]), dot(tok_ref[...], wbc_ref[...]), taps)
    bc_ref[...] = bc
    bt_ref[...] = bc.astype(F32).T.astype(BF16)
    shard_states(w_ref[...], prm[0:CONV], 0, 0, tok_ref, halo_ref, tail_ref, bt_ref, xa_ref, msg_ref)


def others_kernel(c_ref, tok_ref, halo_ref, tail_ref, bt_ref, bc_ref, logp_ref, own_msg_ref, own_prm_ref, *rest):
    here, there = rest[0 : SHARDS - 1], rest[SHARDS - 1 : 2 * SHARDS - 2]
    xa_ref, msg_ref, seen_ref, prm_ref, w_ref = rest[2 * SHARDS - 2 :]
    core = c_ref[0]
    seen_ref[:, 0:LANES] = bc_ref[...]
    seen_ref[:, LANES:] = logp_ref[...]
    half, wide = w_ref.shape[0] // 2, w_ref.shape[1]
    msg_ref[...] = own_msg_ref[...]
    prm_ref[:, 0:wide] = own_prm_ref[0:8]
    for r in range(1, SHARDS):
        a, b = here[r - 1][0:half], there[r - 1][0:half]
        w_ref[0:half] = jnp.where(core == 0, a, b)
        w_ref[half : 2 * half] = jnp.where(core == 0, b, a)
        prm_ref[:, r * wide : (r + 1) * wide] = here[r - 1][half : half + 8]
        taps = here[r - 1][half : half + 8].astype(F32)
        shard_states(w_ref[...], taps, r, (r - 1) * wide, tok_ref, halo_ref, tail_ref, bt_ref, xa_ref, msg_ref)


def scan_kernel(s_ref, out_ref):
    def step(k, carry):
        out_ref[k] = carry.astype(BF16)
        extra = s_ref[k, PART : PART + 8].astype(F32)
        return carry * jnp.exp(extra[0:1] + extra[1:2]) + s_ref[k, 0:PART].astype(F32)

    lax.fori_loop(0, s_ref.shape[0], step, jnp.zeros((PART, LANES), F32), unroll=8)


def intra_kernel(xa0_ref, xa1_ref, seen_ref, prm_ref, y_ref):
    length, wide = xa0_ref.shape
    blocks = length // BLOCK
    lower_block = lower_ones(BLOCK)
    keep = iota((BLOCK, BLOCK), 0) >= iota((BLOCK, BLOCK), 1)
    left = iota((BLOCK, LANES), 1) < LANES // 2
    bc = seen_ref[:, 0:LANES]
    bt = bc.astype(F32).T.astype(BF16)
    logp = seen_ref[:, LANES:]
    scale = scale_of(logp.astype(F32))
    scale_t = scale.T
    span = [slice(b * BLOCK, (b + 1) * BLOCK) for b in range(blocks)]
    cums = [dot(lower_block, logp[span[b]]) for b in range(blocks)]
    cums_t = [cum.T for cum in cums]
    reads = [bc[span[b]][:, STATE:] for b in range(blocks)]
    writes_t = [bt[0:STATE, b * BLOCK : (b + 1) * BLOCK] for b in range(blocks)]
    scores = [jnp.where(keep, dot(reads[b], writes_t[b]), 0.0) for b in range(blocks)]
    factors = hi_lo(
        jnp.concatenate(
            [jnp.exp(cum) for cum in cums[1:]]
            + [jnp.exp(cums[b][BLOCK - 1 :] - cums[b]) * scale[span[b]] for b in range(blocks - 1)],
            axis=0,
        )
    )
    for j in range(SHARDS * wide // LANES):
        lanes = slice(j * LANES, (j + 1) * LANES)
        spreads = dot(factors, spread(j * LANES, LANES))
        skip = prm_ref[CONV + 1 : CONV + 2, lanes].astype(F32)
        state = None
        for b in range(blocks):
            if j * LANES < wide:
                xb = xa0_ref[span[b], lanes]
            else:
                xb = xa1_ref[span[b], j * LANES - wide : (j + 1) * LANES - wide]
            parts = []
            for h in (2 * j, 2 * j + 1):
                seg = cums[b][:, h : h + 1] - cums_t[b][h : h + 1, :]
                decay = jnp.exp(jnp.minimum(seg, 0.0))
                weights = decay * (scores[b] * scale_t[h : h + 1, span[b]])
                parts.append(weights.astype(BF16))
            zero = jnp.zeros_like(xb)
            split = jnp.concatenate([jnp.where(left, xb, zero), jnp.where(left, zero, xb)], axis=0)
            y = dot(jnp.concatenate(parts, axis=1), split) + skip * xb.astype(F32)
            if state is not None:
                enter = spreads[(b - 1) * BLOCK : b * BLOCK]
                y = y + enter * dot(reads[b], state.astype(BF16))
            if b + 1 < blocks:
                leave = spreads[(blocks - 1 + b) * BLOCK : (blocks + b) * BLOCK]
                fresh = dot(writes_t[b], (xb.astype(F32) * leave).astype(BF16))
                state = fresh if state is None else fresh + enter[BLOCK - 1 :] * state
            y_ref[span[b], lanes] = y.astype(BF16)


def gate_kernel(c_ref, tok_ref, seen_ref, y_ref, wz0_ref, wo0_ref, *rest):
    here, there = rest[0 : SHARDS - 1], rest[SHARDS - 1 : 2 * SHARDS - 2]
    yg_ref, eg_ref, wo_ref, wz_ref = rest[2 * SHARDS - 2 :]
    core = c_ref[0]
    depth, wide = wz0_ref.shape
    half, q = depth // 2, wide // 2
    length = tok_ref.shape[0]
    wo_ref[0:wide] = wo0_ref[...]
    grow = hi_lo(jnp.exp(dot(lower_ones(length), seen_ref[:, LANES:])))
    for r in range(SHARDS):
        if r == 0:
            wz_ref[...] = wz0_ref[...]
        else:
            a, b = here[r - 1], there[r - 1]
            wz_ref[0:half] = jnp.where(core == 0, a[0:half], b[0:half])
            wz_ref[half:depth] = jnp.where(core == 0, b[0:half], a[0:half])
            for s in range(2):
                part = slice(half + s * q, half + (s + 1) * q)
                lanes = slice(s * wide, (s + 1) * wide)
                wo_ref[r * wide : r * wide + q, lanes] = jnp.where(core == 0, a[part], b[part])
                wo_ref[r * wide + q : (r + 1) * wide, lanes] = jnp.where(core == 0, b[part], a[part])
        lanes = slice(r * wide, (r + 1) * wide)
        gate = silu(dot(tok_ref[...], wz_ref[...]).astype(BF16).astype(F32))
        yg_ref[:, lanes] = (y_ref[:, lanes].astype(F32) * gate).astype(BF16)
        eg_ref[:, lanes] = (dot(grow, spread(r * wide, wide)) * gate).astype(BF16)


def final_rows(start, back_ref, seen_ref, yg_ref, eg_ref, gain_ref, wo_ref, normed_ref):
    length, width = normed_ref.shape
    rows = pl.ds(pl.multiple_of(start, length), length)
    read = seen_ref[rows, STATE : 2 * STATE]
    shape = (2 * LANES, LANES)
    same_head = ones_where(((iota(shape, 0) & (LANES - 1)) >> 6) == (iota(shape, 1) >> 6))
    parts = STATE // PART
    for j in range(width // LANES):
        lanes = slice(j * LANES, (j + 1) * LANES)
        carry = jnp.concatenate([back_ref[j * parts + q] for q in range(parts)], axis=0)
        v = yg_ref[rows, lanes].astype(F32) + eg_ref[rows, lanes].astype(F32) * dot(read, carry)
        mean = dot(two_terms(v * v), same_head) * (1.0 / 64.0)
        gain = gain_ref[CONV : CONV + 1, lanes].astype(F32)
        normed_ref[:, lanes] = (v * lax.rsqrt(mean + 1e-05) * gain).astype(BF16)
    return dot(normed_ref[...], wo_ref[...]).astype(BF16)


def final_send_kernel(c_ref, back_ref, seen_ref, yg_ref, eg_ref, gain_ref, wo_ref, out_ref, normed_ref):
    start = (1 - c_ref[0]) * normed_ref.shape[0]
    out_ref[...] = final_rows(start, back_ref, seen_ref, yg_ref, eg_ref, gain_ref, wo_ref, normed_ref)


def final_own_kernel(c_ref, back_ref, seen_ref, yg_ref, eg_ref, gain_ref, wo_ref, out_ref, normed_ref):
    start = c_ref[0] * normed_ref.shape[0]
    out_ref[...] = final_rows(start, back_ref, seen_ref, yg_ref, eg_ref, gain_ref, wo_ref, normed_ref)


def join_kernel(c_ref, own_ref, got_ref, out_ref, sems):
    core = c_ref[0]
    copies = [
        pltpu.make_async_copy(own_ref, out_ref.at[core], sems.at[0]),
        pltpu.make_async_copy(got_ref, out_ref.at[1 - core], sems.at[1]),
    ]
    for copy in copies:
        copy.start()
    for copy in copies:
        copy.wait()


VMEM = pl.BlockSpec(memory_space=pltpu.VMEM)
SMEM = pl.BlockSpec(memory_space=pltpu.SMEM)
HBM = pl.BlockSpec(memory_space=pltpu.HBM)
ANY = pl.BlockSpec()


def call(kernel, outs, args, specs, out_specs=None, scratch=(), flops=0, mib=24):
    return pl.pallas_call(
        kernel,
        out_shape=[jax.ShapeDtypeStruct(shape, dtype) for shape, dtype in outs],
        in_specs=specs,
        out_specs=out_specs or [VMEM] * len(outs),
        scratch_shapes=list(scratch),
        compiler_params=pltpu.CompilerParams(vmem_limit_bytes=mib * 2**20),
        cost_estimate=pl.CostEstimate(flops=flops, bytes_accessed=2**20, transcendentals=0),
    )(*args)


def around(value, axis, steps):
    count = lax.axis_size(axis)
    return lax.ppermute(value, axis, [(k, (k + steps) % count) for k in range(count)])


def padded(value, above, rows, columns=None):
    columns = value.shape[1] if columns is None else columns
    return lax.pad(
        value, jnp.zeros((), value.dtype), [(above, rows - above - value.shape[0], 0), (0, columns - value.shape[1], 0)]
    )


def layer(tokens, log_forget_rate, w_x, w_z, w_bc, conv_x, conv_bc, skip, gain, w_out):
    core, across = lax.axis_index("seq_2"), lax.axis_index("mix")
    core_s, across_s = core.astype(jnp.int32)[None], across.astype(jnp.int32)[None]
    _, length, depth = tokens.shape
    wide = w_x.shape[1]
    width = wide * SHARDS
    half = depth // 2
    chips = lax.axis_size(CHIPS)
    both = 2 * length
    logs = jnp.swapaxes(log_forget_rate, 1, 2)
    parts = width // LANES * (STATE // PART)

    low = core == 0
    extra = (
        padded(conv_x, 0, 16)
        + padded(gain[None], CONV, 16)
        + padded(jnp.repeat(skip, wide // skip.shape[0])[None], CONV + 1, 16)
        + padded(conv_bc, 8, 16, wide)
    )
    first = padded(jnp.where(low, w_x[:half], w_x[half:]), 0, half + 16) + padded(extra, half, half + 16)
    x_here = [around(first, "mix", r) for r in (2, 1, 3)]
    x_here = [x_here[1], x_here[0], x_here[2]]
    got = around(tokens, "seq_2", 1)
    got_log = around(logs, "seq_2", 1)
    edge = tokens[:, length - HALO :]
    halo = [lax.ppermute(edge, SEQ, [(2 * k + 1, 2 * k + 2 + to) for k in range(chips - 1)]) for to in range(2)]
    tok, logp, tail, totals = call(
        decay_kernel,
        [
            ((both, depth), BF16),
            ((both, LANES), BF16),
            ((both, LANES), BF16),
            ((8, width), BF16),
        ],
        (core_s, across_s, tokens, logs, got, got_log),
        [SMEM, SMEM, ANY, ANY, VMEM, VMEM],
        flops=10**9,
    )
    halo, bc, bt, xa0, own_msg = call(
        own_kernel,
        [
            ((HALO, depth), BF16),
            ((both, 2 * STATE), BF16),
            ((2 * STATE, both), BF16),
            ((both, wide), BF16),
            ((parts, PART + 8, LANES), BF16),
        ],
        (core_s, tok, *halo, tail, totals, w_bc, w_x, extra),
        [SMEM] + [VMEM] * 5 + [ANY] * 2 + [VMEM],
        flops=10**9,
    )
    x_there = [around(part, "seq_2", 1) for part in x_here]
    xa1, msg, seen, prm = call(
        others_kernel,
        [((both, width - wide), BF16), ((parts, PART + 8, LANES), BF16), ((both, 2 * LANES), BF16), ((8, width), BF16)],
        (core_s, tok, halo, tail, bt, bc, logp, own_msg, extra, *x_here, *x_there),
        [SMEM] + [VMEM] * 14,
        scratch=[pltpu.VMEM((depth, wide), BF16)],
        flops=10**9,
    )
    arrived = lax.all_to_all(msg, CHIPS, 0, 0)
    w_z, w_out, _ = lax.optimization_barrier((w_z, w_out, msg))
    out_half = jnp.where(low, w_out[: wide // 2], w_out[wide // 2 :])
    second = (
        padded(jnp.where(low, w_z[:half], w_z[half:]), 0, depth)
        + padded(out_half[:, :wide], half, depth)
        + padded(out_half[:, wide:], half + wide // 2, depth)
    )
    z_here = [around(second, "mix", r) for r in (2, 1, 3)]
    z_here = [z_here[1], z_here[0], z_here[2]]
    (carries,) = call(scan_kernel, [((parts, PART, LANES), BF16)], (arrived,), [VMEM], flops=10**7)
    back = lax.all_to_all(carries, CHIPS, 0, 0)
    (y,) = call(intra_kernel, [((both, width), BF16)], (xa0, xa1, seen, prm), [VMEM] * 4, flops=2 * 10**9)
    z_here, y = lax.optimization_barrier((z_here, y))
    z_there = [around(part, "seq_2", 1) for part in z_here]
    y, back = lax.optimization_barrier((y, back))
    yg, eg, wo = call(
        gate_kernel,
        [((both, width), BF16), ((both, width), BF16), ((width, depth), BF16)],
        (core_s, tok, seen, y, w_z, w_out, *z_here, *z_there),
        [SMEM] + [ANY] * 11,
        scratch=[pltpu.VMEM((depth, wide), BF16)],
        flops=2 * 10**9,
    )
    ends = (core_s, back, seen, yg, eg, prm, wo)
    specs = [SMEM, VMEM, ANY, VMEM, VMEM, VMEM, VMEM]
    scratch = [pltpu.VMEM((length, width), BF16)]
    (away,) = call(final_send_kernel, [((length, depth), BF16)], ends, specs, scratch=scratch, flops=10**9)
    back_home = around(away, "seq_2", 1)
    (home,) = call(final_own_kernel, [((length, depth), BF16)], ends, specs, scratch=scratch, flops=10**9)
    (mixed,) = call(
        join_kernel,
        [((2, length, depth), BF16)],
        (core_s, home, back_home),
        [SMEM, VMEM, VMEM],
        out_specs=[HBM],
        scratch=[pltpu.SemaphoreType.DMA((2,))],
    )
    return mixed


def solution(mesh):
    finer = Mesh(
        mesh.devices.reshape(8, 4, 2, mesh.shape["mix"]), ("seq_0", "seq_1", "seq_2", "mix")
    )
    placed = (
        P("mix", SEQ, None),
        P("mix", SEQ, None),
        P(None, "mix"),
        P(None, "mix"),
        P(),
        P(None, "mix"),
        P(),
        P("mix"),
        P("mix"),
        P("mix", None),
    )
    return jax.shard_map(layer, mesh=finer, in_specs=placed, out_specs=P("mix", SEQ, None), check_vma=False)
```

```python
import jax
import jax.numpy as jnp
from jax import lax
from jax.experimental import pallas as pl
from jax.experimental.pallas import tpu as pltpu
from jax.sharding import Mesh
from jax.sharding import PartitionSpec as P


F32, BF16 = jnp.float32, jnp.bfloat16
CHIPS = ("seq_0", "seq_1")
SEQ = ("seq_0", "seq_1", "seq_2")
STATE = 64
CONV = 4
BLOCK = 128
LANES = 128
HALO = 16
SHARDS = 4
HEADS = 16
PART = 16


def dot(a, b):
    return jnp.dot(a, b, preferred_element_type=F32)


def iota(shape, axis):
    return lax.broadcasted_iota(jnp.int32, shape, axis)


def ones_where(mask):
    return jnp.where(mask, 1.0, 0.0).astype(BF16)


def two_terms(value):
    high = value.astype(BF16)
    low = (value - high.astype(F32)).astype(BF16)
    return jnp.concatenate([high, low], axis=-1)


def hi_lo(value):
    value = jnp.where(iota(value.shape, 1) < HEADS, value, 0.0)
    high = value.astype(BF16).astype(F32)
    return (high + pltpu.roll(value - high, HEADS, 1)).astype(BF16)


def lower_ones(size):
    return ones_where(iota((size, size), 0) >= iota((size, size), 1))


def spread(start, width):
    shape = (LANES, width)
    row = iota(shape, 0)
    return ones_where(((row & (HEADS - 1)) == ((iota(shape, 1) + start) >> 6)) & (row < 2 * HEADS))


def scale_of(rate):
    z = 2.0 * rate
    series = z * (
        1.0
        + z * (1 / 2 + z * (1 / 6 + z * (1 / 24 + z * (1 / 120 + z * (1 / 720)))))
    )
    return jnp.sqrt(jnp.maximum(-jnp.where(z > -0.25, series, jnp.exp(z) - 1.0), 0.0))


def silu(value):
    return value * jax.nn.sigmoid(value)


def conv_silu(halo_rows, rows, taps):
    rows = jnp.concatenate([halo_rows, rows], axis=0).astype(BF16).astype(F32)
    total = taps[CONV - 1 : CONV] * rows
    for back in range(1, CONV):
        total = total + taps[CONV - 1 - back : CONV - back] * pltpu.roll(rows, back, 0)
    return silu(total[HALO:]).astype(BF16)


def shard_states(weight, taps, r, at, tok_ref, halo_ref, tail_ref, bt_ref, xa_ref, msg_ref):
    wide = weight.shape[1]
    xa = conv_silu(dot(halo_ref[...], weight), dot(tok_ref[...], weight), taps)
    xa_ref[:, at : at + wide] = xa
    tail = dot(tail_ref[...], spread(r * wide, wide))
    state = dot(bt_ref[0:STATE, :], (xa.astype(F32) * tail).astype(BF16)).astype(BF16)
    for p in range(wide // LANES):
        for q in range(STATE // PART):
            at_piece = (r * (wide // LANES) + p) * (STATE // PART) + q
            msg_ref[at_piece, 0:PART] = state[q * PART : (q + 1) * PART, p * LANES : (p + 1) * LANES]


def decay_kernel(c_ref, x_ref, tokens_ref, log_ref, got_ref, got_log_ref, tok_ref, logp_ref, tail_ref, extra_ref):
    core, mine = c_ref[0], x_ref[0]
    heads, length = log_ref.shape[1:]
    here = pl.multiple_of(core * length, length)
    there = pl.multiple_of((1 - core) * length, length)
    tok_ref[pl.ds(here, length)] = tokens_ref[core]
    tok_ref[pl.ds(there, length)] = got_ref[core]
    per = heads // SHARDS
    shape = (LANES, heads)
    rel = iota(shape, 0)
    source = per * ((mine - rel // per + SHARDS) & (SHARDS - 1)) + rel % per
    order = ones_where((iota(shape, 1) == source) & (rel < heads))
    a, b = log_ref[core], got_log_ref[core]
    logs = jnp.concatenate([jnp.where(core == 0, a, b), jnp.where(core == 0, b, a)], axis=1)
    rate = dot(order, logs).T
    logp = rate.astype(BF16)
    logp_ref[...] = logp
    cum = dot(lower_ones(2 * length), logp)
    total = cum[2 * length - 1 :]
    tail_ref[...] = hi_lo(jnp.exp(total - cum) * scale_of(rate))
    width = extra_ref.shape[1]
    total_x = dot(hi_lo(jnp.broadcast_to(total, (8, LANES))), spread(0, width))
    high = total_x.astype(BF16).astype(F32)
    row = iota((8, width), 0)
    extra_ref[...] = jnp.where(row == 0, high, jnp.where(row == 1, total_x - high, 0.0)).astype(BF16)


def own_kernel(
    c_ref, tok_ref, h0_ref, h1_ref, tail_ref, extra_ref, wbc_ref, w_ref, prm_ref,
    halo_ref, bc_ref, bt_ref, xa_ref, msg_ref,
):
    core = c_ref[0]
    halo_ref[...] = h0_ref[core] + h1_ref[core]
    extra = extra_ref[...]
    parts = STATE // PART
    for j in range(extra.shape[1] // LANES):
        for q in range(parts):
            msg_ref[j * parts + q, PART : PART + 8] = extra[:, j * LANES : (j + 1) * LANES]
    prm = prm_ref[...].astype(F32)
    taps = prm[8 : 8 + CONV, 0 : 2 * STATE]
    bc = conv_silu(dot(halo_ref[...], wbc_ref[...]), dot(tok_ref[...], wbc_ref[...]), taps)
    bc_ref[...] = bc
    bt_ref[...] = bc.astype(F32).T.astype(BF16)
    shard_states(w_ref[...], prm[0:CONV], 0, 0, tok_ref, halo_ref, tail_ref, bt_ref, xa_ref, msg_ref)


def others_kernel(c_ref, tok_ref, halo_ref, tail_ref, bt_ref, bc_ref, logp_ref, own_msg_ref, own_prm_ref, *rest):
    here, there = rest[0 : SHARDS - 1], rest[SHARDS - 1 : 2 * SHARDS - 2]
    xa_ref, msg_ref, seen_ref, prm_ref, w_ref = rest[2 * SHARDS - 2 :]
    core = c_ref[0]
    seen_ref[:, 0:LANES] = bc_ref[...]
    seen_ref[:, LANES:] = logp_ref[...]
    half, wide = w_ref.shape[0] // 2, w_ref.shape[1]
    msg_ref[...] = own_msg_ref[...]
    prm_ref[:, 0:wide] = own_prm_ref[0:8]
    for r in range(1, SHARDS):
        a, b = here[r - 1][0:half], there[r - 1][0:half]
        w_ref[0:half] = jnp.where(core == 0, a, b)
        w_ref[half : 2 * half] = jnp.where(core == 0, b, a)
        prm_ref[:, r * wide : (r + 1) * wide] = here[r - 1][half : half + 8]
        taps = here[r - 1][half : half + 8].astype(F32)
        shard_states(w_ref[...], taps, r, (r - 1) * wide, tok_ref, halo_ref, tail_ref, bt_ref, xa_ref, msg_ref)


def scan_kernel(s_ref, out_ref):
    def step(k, carry):
        out_ref[k] = carry.astype(BF16)
        extra = s_ref[k, PART : PART + 8].astype(F32)
        return carry * jnp.exp(extra[0:1] + extra[1:2]) + s_ref[k, 0:PART].astype(F32)

    lax.fori_loop(0, s_ref.shape[0], step, jnp.zeros((PART, LANES), F32), unroll=8)


def intra_kernel(xa0_ref, xa1_ref, seen_ref, prm_ref, y_ref):
    length, wide = xa0_ref.shape
    blocks = length // BLOCK
    lower_block = lower_ones(BLOCK)
    keep = iota((BLOCK, BLOCK), 0) >= iota((BLOCK, BLOCK), 1)
    left = iota((BLOCK, LANES), 1) < LANES // 2
    bc = seen_ref[:, 0:LANES]
    bt = bc.astype(F32).T.astype(BF16)
    logp = seen_ref[:, LANES:]
    scale = scale_of(logp.astype(F32))
    scale_t = scale.T
    span = [slice(b * BLOCK, (b + 1) * BLOCK) for b in range(blocks)]
    cums = [dot(lower_block, logp[span[b]]) for b in range(blocks)]
    cums_t = [cum.T for cum in cums]
    reads = [bc[span[b]][:, STATE:] for b in range(blocks)]
    writes_t = [bt[0:STATE, b * BLOCK : (b + 1) * BLOCK] for b in range(blocks)]
    scores = [jnp.where(keep, dot(reads[b], writes_t[b]), 0.0) for b in range(blocks)]
    factors = hi_lo(
        jnp.concatenate(
            [jnp.exp(cum) for cum in cums[1:]]
            + [jnp.exp(cums[b][BLOCK - 1 :] - cums[b]) * scale[span[b]] for b in range(blocks - 1)],
            axis=0,
        )
    )
    for j in range(SHARDS * wide // LANES):
        lanes = slice(j * LANES, (j + 1) * LANES)
        spreads = dot(factors, spread(j * LANES, LANES))
        skip = prm_ref[CONV + 1 : CONV + 2, lanes].astype(F32)
        state = None
        for b in range(blocks):
            if j * LANES < wide:
                xb = xa0_ref[span[b], lanes]
            else:
                xb = xa1_ref[span[b], j * LANES - wide : (j + 1) * LANES - wide]
            parts = []
            for h in (2 * j, 2 * j + 1):
                seg = cums[b][:, h : h + 1] - cums_t[b][h : h + 1, :]
                decay = jnp.exp(jnp.minimum(seg, 0.0))
                weights = decay * (scores[b] * scale_t[h : h + 1, span[b]])
                parts.append(weights.astype(BF16))
            zero = jnp.zeros_like(xb)
            split = jnp.concatenate([jnp.where(left, xb, zero), jnp.where(left, zero, xb)], axis=0)
            y = dot(jnp.concatenate(parts, axis=1), split) + skip * xb.astype(F32)
            if state is not None:
                enter = spreads[(b - 1) * BLOCK : b * BLOCK]
                y = y + enter * dot(reads[b], state.astype(BF16))
            if b + 1 < blocks:
                leave = spreads[(blocks - 1 + b) * BLOCK : (blocks + b) * BLOCK]
                fresh = dot(writes_t[b], (xb.astype(F32) * leave).astype(BF16))
                state = fresh if state is None else fresh + enter[BLOCK - 1 :] * state
            y_ref[span[b], lanes] = y.astype(BF16)


def gate_kernel(c_ref, tok_ref, seen_ref, y_ref, wz0_ref, wo0_ref, *rest):
    here, there = rest[0 : SHARDS - 1], rest[SHARDS - 1 : 2 * SHARDS - 2]
    yg_ref, eg_ref, wo_ref, wz_ref = rest[2 * SHARDS - 2 :]
    core = c_ref[0]
    depth, wide = wz0_ref.shape
    half, q = depth // 2, wide // 2
    length = tok_ref.shape[0]
    wo_ref[0:wide] = wo0_ref[...]
    grow = hi_lo(jnp.exp(dot(lower_ones(length), seen_ref[:, LANES:])))
    for r in range(SHARDS):
        if r == 0:
            wz_ref[...] = wz0_ref[...]
        else:
            a, b = here[r - 1], there[r - 1]
            wz_ref[0:half] = jnp.where(core == 0, a[0:half], b[0:half])
            wz_ref[half:depth] = jnp.where(core == 0, b[0:half], a[0:half])
            for s in range(2):
                part = slice(half + s * q, half + (s + 1) * q)
                lanes = slice(s * wide, (s + 1) * wide)
                wo_ref[r * wide : r * wide + q, lanes] = jnp.where(core == 0, a[part], b[part])
                wo_ref[r * wide + q : (r + 1) * wide, lanes] = jnp.where(core == 0, b[part], a[part])
        lanes = slice(r * wide, (r + 1) * wide)
        gate = silu(dot(tok_ref[...], wz_ref[...]).astype(BF16).astype(F32))
        yg_ref[:, lanes] = (y_ref[:, lanes].astype(F32) * gate).astype(BF16)
        eg_ref[:, lanes] = (dot(grow, spread(r * wide, wide)) * gate).astype(BF16)


def final_rows(start, back_ref, seen_ref, yg_ref, eg_ref, gain_ref, wo_ref, normed_ref):
    length, width = normed_ref.shape
    rows = pl.ds(pl.multiple_of(start, length), length)
    read = seen_ref[rows, STATE : 2 * STATE]
    shape = (2 * LANES, LANES)
    same_head = ones_where(((iota(shape, 0) & (LANES - 1)) >> 6) == (iota(shape, 1) >> 6))
    parts = STATE // PART
    for j in range(width // LANES):
        lanes = slice(j * LANES, (j + 1) * LANES)
        carry = jnp.concatenate([back_ref[j * parts + q] for q in range(parts)], axis=0)
        v = yg_ref[rows, lanes].astype(F32) + eg_ref[rows, lanes].astype(F32) * dot(read, carry)
        mean = dot(two_terms(v * v), same_head) * (1.0 / 64.0)
        gain = gain_ref[CONV : CONV + 1, lanes].astype(F32)
        normed_ref[:, lanes] = (v * lax.rsqrt(mean + 1e-05) * gain).astype(BF16)
    return dot(normed_ref[...], wo_ref[...]).astype(BF16)


def final_send_kernel(c_ref, back_ref, seen_ref, yg_ref, eg_ref, gain_ref, wo_ref, out_ref, normed_ref):
    start = (1 - c_ref[0]) * normed_ref.shape[0]
    out_ref[...] = final_rows(start, back_ref, seen_ref, yg_ref, eg_ref, gain_ref, wo_ref, normed_ref)


def final_own_kernel(c_ref, back_ref, seen_ref, yg_ref, eg_ref, gain_ref, wo_ref, out_ref, normed_ref):
    start = c_ref[0] * normed_ref.shape[0]
    out_ref[...] = final_rows(start, back_ref, seen_ref, yg_ref, eg_ref, gain_ref, wo_ref, normed_ref)


def join_kernel(c_ref, own_ref, got_ref, out_ref, sems):
    core = c_ref[0]
    copies = [
        pltpu.make_async_copy(own_ref, out_ref.at[core], sems.at[0]),
        pltpu.make_async_copy(got_ref, out_ref.at[1 - core], sems.at[1]),
    ]
    for copy in copies:
        copy.start()
    for copy in copies:
        copy.wait()


VMEM = pl.BlockSpec(memory_space=pltpu.VMEM)
SMEM = pl.BlockSpec(memory_space=pltpu.SMEM)
HBM = pl.BlockSpec(memory_space=pltpu.HBM)
ANY = pl.BlockSpec()


def call(kernel, outs, args, specs, out_specs=None, scratch=(), flops=0, mib=24):
    return pl.pallas_call(
        kernel,
        out_shape=[jax.ShapeDtypeStruct(shape, dtype) for shape, dtype in outs],
        in_specs=specs,
        out_specs=out_specs or [VMEM] * len(outs),
        scratch_shapes=list(scratch),
        compiler_params=pltpu.CompilerParams(vmem_limit_bytes=mib * 2**20),
        cost_estimate=pl.CostEstimate(flops=flops, bytes_accessed=2**20, transcendentals=0),
    )(*args)


def around(value, axis, steps):
    count = lax.axis_size(axis)
    return lax.ppermute(value, axis, [(k, (k + steps) % count) for k in range(count)])


def padded(value, above, rows, columns=None):
    columns = value.shape[1] if columns is None else columns
    return lax.pad(
        value, jnp.zeros((), value.dtype), [(above, rows - above - value.shape[0], 0), (0, columns - value.shape[1], 0)]
    )


def layer(tokens, log_forget_rate, w_x, w_z, w_bc, conv_x, conv_bc, skip, gain, w_out):
    core, across = lax.axis_index("seq_2"), lax.axis_index("mix")
    core_s, across_s = core.astype(jnp.int32)[None], across.astype(jnp.int32)[None]
    _, length, depth = tokens.shape
    wide = w_x.shape[1]
    width = wide * SHARDS
    half = depth // 2
    chips = lax.axis_size(CHIPS)
    both = 2 * length
    logs = jnp.swapaxes(log_forget_rate, 1, 2)
    parts = width // LANES * (STATE // PART)

    low = core == 0
    extra = (
        padded(conv_x, 0, 16)
        + padded(gain[None], CONV, 16)
        + padded(jnp.repeat(skip, wide // skip.shape[0])[None], CONV + 1, 16)
    )
    first = padded(jnp.where(low, w_x[:half], w_x[half:]), 0, half + 8) + padded(extra[:8], half, half + 8)
    x_here = [around(first, "mix", r) for r in (2, 1, 3)]
    x_here = [x_here[1], x_here[0], x_here[2]]
    got = around(tokens, "seq_2", 1)
    got_log = around(logs, "seq_2", 1)
    own_taps, _ = lax.optimization_barrier((conv_bc, first))
    own_extra = extra + padded(own_taps, 8, 16, wide)
    edge = tokens[:, length - HALO :]
    halo = [lax.ppermute(edge, SEQ, [(2 * k + 1, 2 * k + 2 + to) for k in range(chips - 1)]) for to in range(2)]
    tok, logp, tail, totals = call(
        decay_kernel,
        [
            ((both, depth), BF16),
            ((both, LANES), BF16),
            ((both, LANES), BF16),
            ((8, width), BF16),
        ],
        (core_s, across_s, tokens, logs, got, got_log),
        [SMEM, SMEM, ANY, ANY, VMEM, VMEM],
        flops=10**9,
    )
    halo, bc, bt, xa0, own_msg = call(
        own_kernel,
        [
            ((HALO, depth), BF16),
            ((both, 2 * STATE), BF16),
            ((2 * STATE, both), BF16),
            ((both, wide), BF16),
            ((parts, PART + 8, LANES), BF16),
        ],
        (core_s, tok, *halo, tail, totals, w_bc, w_x, own_extra),
        [SMEM] + [VMEM] * 5 + [ANY] * 2 + [VMEM],
        flops=10**9,
    )
    x_there = [around(part, "seq_2", 1) for part in x_here]
    xa1, msg, seen, prm = call(
        others_kernel,
        [((both, width - wide), BF16), ((parts, PART + 8, LANES), BF16), ((both, 2 * LANES), BF16), ((8, width), BF16)],
        (core_s, tok, halo, tail, bt, bc, logp, own_msg, extra, *x_here, *x_there),
        [SMEM] + [VMEM] * 14,
        scratch=[pltpu.VMEM((depth, wide), BF16)],
        flops=10**9,
    )
    arrived = lax.all_to_all(msg, CHIPS, 0, 0)
    w_z, w_out, _ = lax.optimization_barrier((w_z, w_out, msg))
    out_half = jnp.where(low, w_out[: wide // 2], w_out[wide // 2 :])
    second = (
        padded(jnp.where(low, w_z[:half], w_z[half:]), 0, depth)
        + padded(out_half[:, :wide], half, depth)
        + padded(out_half[:, wide:], half + wide // 2, depth)
    )
    z_here = [around(second, "mix", r) for r in (2, 1, 3)]
    z_here = [z_here[1], z_here[0], z_here[2]]
    (carries,) = call(scan_kernel, [((parts, PART, LANES), BF16)], (arrived,), [VMEM], flops=10**7)
    back = lax.all_to_all(carries, CHIPS, 0, 0)
    (y,) = call(intra_kernel, [((both, width), BF16)], (xa0, xa1, seen, prm), [VMEM] * 4, flops=2 * 10**9)
    z_here, y = lax.optimization_barrier((z_here, y))
    z_there = [around(part, "seq_2", 1) for part in z_here]
    y, back = lax.optimization_barrier((y, back))
    yg, eg, wo = call(
        gate_kernel,
        [((both, width), BF16), ((both, width), BF16), ((width, depth), BF16)],
        (core_s, tok, seen, y, w_z, w_out, *z_here, *z_there),
        [SMEM] + [ANY] * 11,
        scratch=[pltpu.VMEM((depth, wide), BF16)],
        flops=2 * 10**9,
    )
    ends = (core_s, back, seen, yg, eg, prm, wo)
    specs = [SMEM, VMEM, ANY, VMEM, VMEM, VMEM, VMEM]
    scratch = [pltpu.VMEM((length, width), BF16)]
    (away,) = call(final_send_kernel, [((length, depth), BF16)], ends, specs, scratch=scratch, flops=10**9)
    back_home = around(away, "seq_2", 1)
    (home,) = call(final_own_kernel, [((length, depth), BF16)], ends, specs, scratch=scratch, flops=10**9)
    (mixed,) = call(
        join_kernel,
        [((2, length, depth), BF16)],
        (core_s, home, back_home),
        [SMEM, VMEM, VMEM],
        out_specs=[HBM],
        scratch=[pltpu.SemaphoreType.DMA((2,))],
    )
    return mixed


def solution(mesh):
    finer = Mesh(
        mesh.devices.reshape(8, 4, 2, mesh.shape["mix"]), ("seq_0", "seq_1", "seq_2", "mix")
    )
    placed = (
        P("mix", SEQ, None),
        P("mix", SEQ, None),
        P(None, "mix"),
        P(None, "mix"),
        P(),
        P(None, "mix"),
        P(),
        P("mix"),
        P("mix"),
        P("mix", None),
    )
    return jax.shard_map(layer, mesh=finer, in_specs=placed, out_specs=P("mix", SEQ, None), check_vma=False)
```
